32 devices in a mesh: groups: 2 (over x), seq: 16 (over z, y, core).
Axes of the slice: x: 2, y: 2, z: 4, core: 2. Of those that a mesh axis runs over, the one named last changes fastest.
Arguments:
- queries: bfloat16 [4, 128, 8192], P(None, ('groups', 'seq')), parts along dimension 1, may hold values from -16 to 16
- new_keys: bfloat16 [4, 128, 1024], P(None, ('groups', 'seq')), parts along dimension 1, may hold values from -6 to 6
- new_values: bfloat16 [4, 128, 1024], P(None, ('groups', 'seq')), parts along dimension 1, may hold values from -6 to 6
- pool_keys: bfloat16 [2048, 16, 1024], P(('groups', 'seq')), parts along dimension 0, may hold values from -6 to 6
- pool_values: bfloat16 [2048, 16, 1024], P(('groups', 'seq')), parts along dimension 0, may hold values from -6 to 6
- page_table: int32 [128, 16], P(('groups', 'seq')), parts along dimension 0, may hold values from 0 to 63, as said below
- cached_len: int32 [128], P(('groups', 'seq')), parts along dimension 0, may hold values from 1 to 256
- turn_keys: bfloat16 [4, 32, 16, 1024], P(None, ('groups', 'seq')), parts along dimension 1, may hold values from -6 to 6
- turn_values: bfloat16 [4, 32, 16, 1024], P(None, ('groups', 'seq')), parts along dimension 1, may hold values from -6 to 6
- turn_lengths: int32 [32], P('groups'), parts along dimension 0, may hold values from 1 to 80, 768 in all
- turn_slot: int32 [32], P('groups'), parts along dimension 0, may hold values from 0 to 63, as said below
Outputs:
- attended: bfloat16 [4, 128, 8192], P(None, ('groups', 'seq')), parts along dimension 1
- landed_keys: bfloat16 [32, 80, 1024], P(('groups', 'seq')), parts along dimension 0
- landed_values: bfloat16 [32, 80, 1024], P(('groups', 'seq')), parts along dimension 0
The draws below stay inside these ranges and needn't reach their ends.
There are 2 independent parts, one for each index of `groups`. The reference program is written for one: setup_inputs(seed, part) draws one part's arguments, and reference() takes and returns one part's arrays. A program takes and returns all parts, laid end to end along the dimension named above; each array names one. Nothing has to cross between parts.
Inputs may be any that keep to these rules, and one draw needn't show every extreme that they name: `page_table`: the 4 rows of each device's slots together hold every number of 0 to 63 exactly once. `turn_lengths`: they sum to 768; the largest is exactly 80. `turn_slot`: each block of 4 slots holds the slot of exactly one turn.
All inputs are finite; a program needn't handle non-finite values.
Results may differ from the reference program's by a relative error of at most 0.0049.
Values may be sent and summed in bfloat16 or wider, within the bound.
No kernel may reach another device: no remote copies, remote signals or barrier semaphores. Data moves between devices by JAX's collectives and lax.ppermute only.
A program may use at most 128 MiB of HBM per device.

```python
import math
import jax
import jax.numpy as jnp
import numpy as np
from jax import lax

QH = 64
KVH = 8
HD = 128
KV = 1024
PAGE = 16
STEPS = 4
SLOT_DEV = 4
CPAGES = 16
PG_DEV = 4
CHAIN = 16
TURNS = 16
SLOTS = 64
POOL_DEV = 64
POOL = 1024
PPAGES = 64
MOSTT = 80
TTOK = 768


key_level = 5.25


second_level = 5.21875


def draw_page_table(key, part):
    device_keys = jax.random.split(jax.random.fold_in(key, 11), CHAIN)

    def one_device(device_key):
        return jax.random.permutation(device_key, POOL_DEV)
    tables = jax.vmap(one_device)(device_keys)
    return tables.reshape(SLOTS, CPAGES).astype(jnp.int32)


def draw_turn_slot(key, part):
    owner_key, offset_key = jax.random.split(jax.random.fold_in(key, 23))
    owner_ids = jax.random.permutation(owner_key, CHAIN)[:TURNS]
    offsets = jax.random.randint(offset_key, (TURNS,), 0, SLOT_DEV)
    return (owner_ids * SLOT_DEV + offsets).astype(jnp.int32)


def drawn_parts(key):
    group_key, sign_key, level_key = jax.random.split(jax.random.fold_in(key, 77), 3)
    chosen = jax.random.randint(group_key, (SLOTS,), 0, KVH)
    signs = (2 * jax.random.randint(sign_key, (KVH, HD), 0, 2) - 1).astype(jnp.float32)
    levels = jax.random.uniform(level_key, (STEPS, SLOTS, QH // KVH), jnp.float32, 180.0, 320.0)
    return (chosen, signs, levels)


def base_draw(key, shape):
    return jax.random.truncated_normal(key, -6.0, 6.0, shape, jnp.float32)


def draw_queries(key, part):
    chosen, signs, levels = drawn_parts(key)
    group_share = QH // KVH
    base = base_draw(jax.random.fold_in(key, 5), (STEPS, SLOTS, KVH, group_share, HD))
    strength = levels / (key_level * math.sqrt(HD))
    planted = strength[:, :, None, :, None] * signs[None, None, :, None, :]
    in_group = jnp.arange(KVH)[None, :] == chosen[:, None]
    later = jnp.arange(STEPS) >= 1
    using = later[:, None, None] & in_group[None, :, :]
    mixed = jnp.where(using[..., None, None], planted, base)
    return mixed.reshape(STEPS, SLOTS, QH * HD).astype(jnp.bfloat16)


def draw_new_keys(key, part):
    chosen, signs, levels = drawn_parts(key)
    base = base_draw(jax.random.fold_in(key, 6), (STEPS, SLOTS, KVH, HD))
    step_level = jnp.where(jnp.arange(STEPS) == 0, key_level, second_level).astype(jnp.float32)
    planted = step_level[:, None, None, None] * signs[None, None, :, :]
    in_group = jnp.arange(KVH)[None, :] == chosen[:, None]
    early = jnp.arange(STEPS) <= 1
    using = early[:, None, None] & in_group[None, :, :]
    mixed = jnp.where(using[..., None], planted, base)
    return mixed.reshape(STEPS, SLOTS, KV).astype(jnp.bfloat16)


def plant(entries, own_key, least, high):
    place = [jax.random.randint(jax.random.fold_in(own_key, axis), (), 0, length) for axis, length in enumerate(entries.shape)]
    main_axis = entries.shape.index(max(entries.shape))
    next_to = place[:main_axis] + [(place[main_axis] + 1) % entries.shape[main_axis]] + place[main_axis + 1:]
    return entries.at[tuple(place)].set(least).at[tuple(next_to)].set(high)


def block_scale(own_key, extent, cuts, low, top_value):
    factor_of = 1.0
    for dim, parts in cuts:
        heights = jax.random.uniform(jax.random.fold_in(jax.random.fold_in(own_key, 6), dim), (parts,), jnp.float32, low / len(cuts), top_value / len(cuts))
        factor_of = factor_of * jnp.repeat(jnp.exp(heights), extent[dim] // parts).reshape((-1,) + (1,) * (len(extent) - 1 - dim))
    return factor_of


def split_up(number_of, total, most, skew):
    portions = [(1 << 20) // math.isqrt(grade ** skew) + 1 for grade in range(2, number_of + 1)]
    spare, counts = total - most - (number_of - 1), [1] * (number_of - 1)
    while spare > 0:
        movable = [i for i in range(number_of - 1) if counts[i] < most]
        pool, left = sum([portions[i] for i in movable]), spare
        for i in movable:
            addition = min(most - counts[i], max(1, left * portions[i] // pool), spare)
            counts[i] = counts[i] + addition
            spare = spare - addition
    return np.array([most] + counts)


def uneven(rng, count, total, limit, lean):
    if count == 2:
        one = jax.random.randint(rng, (), max(1, total - limit), min(limit, total - 1) + 1)
        return jnp.stack([one, total - one])
    sizes = jnp.asarray(split_up(count, total, limit, lean), jnp.int32)
    twos = (count - 1) // 2
    donor, receiver = sizes[1:1 + 2 * twos:2], sizes[2:2 + 2 * twos:2]
    slack = jnp.minimum(donor - 1, limit - receiver)
    passed = jax.random.randint(jax.random.fold_in(rng, 1), (twos,), 0, 1 << 20) % (slack + 1)
    sizes = sizes.at[1:1 + 2 * twos:2].set(donor - passed).at[2:2 + 2 * twos:2].set(receiver + passed)
    return sizes[jax.random.permutation(jax.random.fold_in(rng, 2), count)]


def normal_values(stream_key, extent, width, reach, pieces=(), held_as=jnp.bfloat16):
    drawn = jax.random.normal(stream_key, extent, jnp.float32) * width
    if len(pieces) > 0:
        drawn = block_scale(stream_key, extent, pieces, -0.22, 0.18) * drawn
    return jnp.clip(drawn, min=-reach, max=reach).astype(held_as)


def setup_inputs(seed: int = 0, part: int = 0) -> dict:
    streams_of = jax.random.split(jax.random.key(seed), 12)
    part_keys = jax.random.split(jax.random.fold_in(streams_of[11], part), 12)
    queries = draw_queries(jax.random.fold_in(jax.random.fold_in(streams_of[11], part), 71), part)
    new_keys = draw_new_keys(jax.random.fold_in(jax.random.fold_in(streams_of[11], part), 71), part)
    new_values = normal_values(part_keys[2], (STEPS, SLOTS, KV), 1.0, 6.0, ((1, 16),))
    pool_keys = normal_values(part_keys[3], (POOL, PAGE, KV), 1.0, 6.0, ((0, 16),))
    pool_values = normal_values(part_keys[4], (POOL, PAGE, KV), 1.0, 6.0, ((0, 16),))
    page_table = draw_page_table(jax.random.fold_in(jax.random.fold_in(streams_of[11], part), 71), part)
    cached_len = plant(jax.random.randint(part_keys[6], (SLOTS,), 1, CPAGES * PAGE + 1), jax.random.fold_in(part_keys[6], 1), 1, CPAGES * PAGE).astype(jnp.int32)
    turn_keys = normal_values(part_keys[7], (PG_DEV, CHAIN, PAGE, KV), 1.0, 6.0, ((1, 16),))
    turn_values = normal_values(part_keys[8], (PG_DEV, CHAIN, PAGE, KV), 1.0, 6.0, ((1, 16),))
    turn_lengths = uneven(part_keys[9], TURNS, TTOK, MOSTT, 2).astype(jnp.int32)
    turn_slot = draw_turn_slot(jax.random.fold_in(jax.random.fold_in(streams_of[11], part), 71), part)
    return {"queries": queries, "new_keys": new_keys, "new_values": new_values, "pool_keys": pool_keys, "pool_values": pool_values, "page_table": page_table, "cached_len": cached_len, "turn_keys": turn_keys, "turn_values": turn_values, "turn_lengths": turn_lengths, "turn_slot": turn_slot}


def reference(queries, new_keys, new_values, pool_keys, pool_values, page_table, cached_len, turn_keys, turn_values, turn_lengths, turn_slot):
    page_counts = (turn_lengths + PAGE - 1) // PAGE
    page_starts = jnp.cumsum(page_counts) - page_counts
    owner_ids = turn_slot // SLOT_DEV
    padding = jnp.zeros((MOSTT, KV), jnp.bfloat16)
    packed_keys = jnp.concatenate([turn_keys.reshape(PPAGES * PAGE, KV), padding], axis=0)
    packed_values = jnp.concatenate([turn_values.reshape(PPAGES * PAGE, KV), padding], axis=0)
    landed_keys = jnp.zeros((CHAIN, MOSTT, KV), jnp.bfloat16)
    landed_values = jnp.zeros((CHAIN, MOSTT, KV), jnp.bfloat16)
    positions = jnp.arange(MOSTT, dtype=jnp.int32)
    for turn_index in range(TURNS):
        first_token = (page_starts[turn_index] * PAGE).astype(jnp.int32)
        keeping = (positions < turn_lengths[turn_index])[:, None]
        piece_keys = lax.dynamic_slice_in_dim(packed_keys, first_token, MOSTT, 0)
        piece_values = lax.dynamic_slice_in_dim(packed_values, first_token, MOSTT, 0)
        landed_keys = landed_keys.at[owner_ids[turn_index]].set(jnp.where(keeping, piece_keys, jnp.zeros_like(piece_keys)))
        landed_values = landed_values.at[owner_ids[turn_index]].set(jnp.where(keeping, piece_values, jnp.zeros_like(piece_values)))
    slot_ids = jnp.arange(SLOTS, dtype=jnp.int32)
    matches = turn_slot[None, :] == slot_ids[:, None]
    fresh_lengths = lax.optimization_barrier(jnp.sum(jnp.where(matches, turn_lengths[None, :], 0), axis=1)).astype(jnp.int32)
    score_scale = 1.0 / math.sqrt(HD)
    group_share = QH // KVH
    token_span = CPAGES * PAGE
    causal_mask = jnp.arange(STEPS)[None, :] <= jnp.arange(STEPS)[:, None]

    def attend_slot(inputs):
        query_rows, key_rows, value_rows, table_row, resident_len, fresh_len, slot_id = inputs
        owner_id = slot_id // SLOT_DEV
        pool_rows = owner_id * POOL_DEV + table_row
        resident_keys = pool_keys[pool_rows].reshape(token_span, KV)
        resident_values = pool_values[pool_rows].reshape(token_span, KV)
        fresh_keys = lax.dynamic_index_in_dim(landed_keys, owner_id, 0, keepdims=False)
        fresh_values = lax.dynamic_index_in_dim(landed_values, owner_id, 0, keepdims=False)
        all_keys = jnp.concatenate([resident_keys, fresh_keys, key_rows], axis=0).astype(jnp.float32).reshape(-1, KVH, HD)
        all_values = jnp.concatenate([resident_values, fresh_values, value_rows], axis=0).astype(jnp.float32).reshape(-1, KVH, HD)
        valid_resident = jnp.broadcast_to((jnp.arange(token_span) < resident_len)[None, :], (STEPS, token_span))
        valid_fresh = jnp.broadcast_to((jnp.arange(MOSTT) < fresh_len)[None, :], (STEPS, MOSTT))
        valid_all = jnp.concatenate([valid_resident, valid_fresh, causal_mask], axis=1)
        query_heads = query_rows.astype(jnp.float32).reshape(STEPS, KVH, group_share, HD)
        scores = jnp.einsum('sgeh,cgh->sgec', query_heads, all_keys) * score_scale
        scores = jnp.where(valid_all[:, None, None, :], scores, -jnp.inf)
        largest = lax.optimization_barrier(jnp.max(scores, axis=-1, keepdims=True))
        weights = jnp.exp(scores - largest)
        weights = weights / lax.optimization_barrier(jnp.sum(weights, axis=-1, keepdims=True))
        mixed = jnp.einsum('sgec,cgh->sgeh', weights, all_values)
        return mixed.reshape(STEPS, QH * HD).astype(jnp.bfloat16)
    per_slot = lax.map(attend_slot, (jnp.swapaxes(queries, 0, 1), jnp.swapaxes(new_keys, 0, 1), jnp.swapaxes(new_values, 0, 1), page_table, cached_len, fresh_lengths, slot_ids))
    attended = jnp.swapaxes(per_slot, 0, 1)
    return (attended, landed_keys, landed_values)
```

```python
import functools
import math

import jax
import jax.numpy as jnp
from jax import lax
from jax.experimental import pallas as pl
from jax.experimental.pallas import tpu as pltpu
from jax.sharding import PartitionSpec as P

QH = 64
KVH = 8
HD = 128
MOSTT = 80


SHARE = QH // KVH
LOG2_SCALE = math.log2(math.e) / math.sqrt(HD)
VMEM = pl.BlockSpec(memory_space=pltpu.VMEM)
SMEM = pl.BlockSpec(memory_space=pltpu.SMEM)
ANY = pl.BlockSpec(memory_space=pl.ANY)
TRANSPOSED = (((1,), (1,)), ((), ()))


def turn_of(meta, turns, page_rows, slots_here, owner):
    def look(t, carry):
        first, start, count, length, slot = carry
        tokens = meta[1 + t]
        pages = (tokens + page_rows - 1) // page_rows
        whose = meta[1 + turns + t]
        mine = whose // slots_here == owner
        return (
            first + pages,
            jnp.where(mine, first, start),
            jnp.where(mine, pages, count),
            jnp.where(mine, tokens, length),
            jnp.where(mine, whose % slots_here, slot),
        )

    zero = jnp.int32(0)
    return lax.fori_loop(0, turns, look, (zero, zero, zero, zero, zero))[1:]


def resident_kernel(
    turns, meta, table, lengths, q, new_k, new_v, pool_k, pool_v,
    out, q_mine, acc_mine, max_mine, sum_mine,
    k_buf, v_buf, o_all, k_sem, v_sem,
):
    steps, slots, _ = out.shape
    pages, page_rows, _ = k_buf.shape[1:]
    pages = pages - 1
    span = (pages + 1) * page_rows
    rows = steps * SHARE

    for r in range(slots):
        def fetch(c, _, r=r):
            page = table[r, c]
            pltpu.make_async_copy(pool_k.at[page], k_buf.at[r, c], k_sem.at[r]).start()
            pltpu.make_async_copy(pool_v.at[page], v_buf.at[r, c], v_sem.at[r]).start()
            return 0

        lax.fori_loop(0, pages, fetch, 0)
    for r in range(slots):
        k_buf[r, pages] = new_k[r]
        v_buf[r, pages] = new_v[r]
    my_slot = turn_of(meta, turns, page_rows, slots, meta[0])[3]
    column = lax.broadcasted_iota(jnp.int32, (rows, span), 1)
    step = lax.broadcasted_iota(jnp.int32, (rows, span), 0) // SHARE
    decode = (column >= pages * page_rows) & (column - pages * page_rows <= step)

    def one_slot(r, _):
        pltpu.make_async_copy(
            pool_k.at[pl.ds(0, pages)], k_buf.at[r, pl.ds(0, pages)], k_sem.at[r]
        ).wait()
        pltpu.make_async_copy(
            pool_v.at[pl.ds(0, pages)], v_buf.at[r, pl.ds(0, pages)], v_sem.at[r]
        ).wait()
        cached = jnp.minimum(lengths[r], pages * page_rows)
        valid = (column < cached) | decode
        for g in range(KVH):
            lanes = pl.ds(g * HD, HD)
            part = pl.ds(g * rows, rows)
            keys = k_buf[r, :, :, lanes].reshape(span, HD)
            values = v_buf[r, :, :, lanes].reshape(span, HD)
            score = lax.dot_general(
                q[r, part, :], keys, TRANSPOSED, preferred_element_type=jnp.float32
            )
            score = jnp.where(valid, score * LOG2_SCALE, -jnp.inf)
            top = jnp.max(score, axis=1, keepdims=True)
            prob = jnp.exp2(score - top)
            total = jnp.sum(prob, axis=1, keepdims=True)
            acc = jnp.dot(prob.astype(jnp.bfloat16), values, preferred_element_type=jnp.float32)
            o_all[pl.ds(r * (KVH * rows) + g * rows, rows), :] = acc / total

            @pl.when(r == my_slot)
            def _():
                acc_mine[part, :] = acc
                max_mine[part, :] = jnp.broadcast_to(top, (rows, HD))
                sum_mine[part, :] = jnp.broadcast_to(total, (rows, HD))

        return 0

    lax.fori_loop(0, slots, one_slot, 0)
    q_mine[...] = q[my_slot]
    for s in range(steps):
        for g in range(KVH):
            for e in range(SHARE):
                row = g * rows + s * SHARE + e
                tile = o_all[pl.ds(row, slots, stride=KVH * rows), :]
                out[s, :, pl.ds((g * SHARE + e) * HD, HD)] = tile.astype(jnp.bfloat16)


def pick_kernel(turns, chain, slots_here, masks, meta, *refs):
    own, twin = refs[0:2], refs[2:4]
    got, got_twin = refs[4:6], refs[6:8]
    outs = refs[8:]
    half = chain // 2
    page_rows = own[0].shape[1]
    me = meta[0]
    for mask, out in zip(masks, outs):
        start, count, _, _ = turn_of(meta, turns, page_rows, slots_here, me ^ mask)
        for slot in range(2):
            here, there = ((own, got), (twin, got_twin))[slot]
            residue = me ^ slot
            page = start + ((residue - start) & (half - 1))
            lap = jnp.minimum(page // chain, own[0].shape[0] - 1)
            near = page % chain == residue

            @pl.when((page < start + count) & near)
            def _(here=here, lap=lap, out=out, slot=slot):
                for kv in range(2):
                    out[slot, kv] = here[kv][lap]

            @pl.when((page < start + count) & jnp.logical_not(near))
            def _(there=there, lap=lap, out=out, slot=slot):
                for kv in range(2):
                    out[slot, kv] = there[kv][lap]


def land_kernel(turns, chain, masks, meta, part_out, q, acc_old, max_old, sum_old, *refs):
    pieces = refs[: len(masks)]
    out, landed_k, landed_v, k_pages, v_pages, o_new = refs[len(masks) :]
    half = chain // 2
    steps, slots, _ = out.shape
    pages, page_rows, width = k_pages.shape
    span = pages * page_rows
    rows = steps * SHARE
    me = meta[0]
    start, count, length, my_slot = turn_of(meta, turns, page_rows, slots, me)
    k_pages[...] = jnp.zeros_like(k_pages)
    v_pages[...] = jnp.zeros_like(v_pages)
    for mask, piece in zip(masks, pieces):
        for slot in range(2):
            place = ((me ^ mask ^ slot) - start) & (half - 1)

            @pl.when(place < count)
            def _(piece=piece, slot=slot, place=place):
                k_pages[place] = piece[slot, 0]
                v_pages[place] = piece[slot, 1]

    token = lax.broadcasted_iota(jnp.int32, (pages, page_rows, width), 0) * page_rows
    token = token + lax.broadcasted_iota(jnp.int32, (pages, page_rows, width), 1)
    keep = token < length
    keys = jnp.where(keep, k_pages[...], jnp.zeros((), jnp.bfloat16))
    values = jnp.where(keep, v_pages[...], jnp.zeros((), jnp.bfloat16))
    keys = keys.reshape(span, width)
    values = values.reshape(span, width)
    landed_k[0] = keys
    landed_v[0] = values
    valid = lax.broadcasted_iota(jnp.int32, (rows, span), 1) < length
    for g in range(KVH):
        part = pl.ds(g * rows, rows)
        score = lax.dot_general(
            q[part, :], keys[:, g * HD : (g + 1) * HD], TRANSPOSED,
            preferred_element_type=jnp.float32,
        )
        score = jnp.where(valid, score * LOG2_SCALE, -jnp.inf)
        before = max_old[part, :]
        top = jnp.maximum(before, jnp.max(score, axis=1, keepdims=True))
        prob = jnp.exp2(score - top[:, :span])
        shrink = jnp.exp2(before - top)
        total = sum_old[part, :] * shrink + jnp.sum(prob, axis=1, keepdims=True)
        acc = jnp.dot(
            prob.astype(jnp.bfloat16), values[:, g * HD : (g + 1) * HD],
            preferred_element_type=jnp.float32,
        )
        o_new[part, :] = (acc_old[part, :] * shrink + acc) / total
    mine = lax.broadcasted_iota(jnp.int32, (slots, HD), 0) == my_slot
    for s in range(steps):
        for g in range(KVH):
            for e in range(SHARE):
                lanes = pl.ds((g * SHARE + e) * HD, HD)
                fresh = o_new[pl.ds(g * rows + s * SHARE + e, 1), :]
                tile = part_out[s, :, lanes].astype(jnp.float32)
                out[s, :, lanes] = jnp.where(mine, fresh, tile).astype(jnp.bfloat16)


def per_device(
    queries, new_keys, new_values, pool_keys, pool_values, page_table, cached_len,
    turn_keys, turn_values, turn_lengths, turn_slot,
):
    chain = lax.axis_size("seq")
    steps, slots, query_width = queries.shape
    page_rows, width = pool_keys.shape[1:]
    pages = page_table.shape[1]
    laps = turn_keys.shape[0]
    turns = turn_lengths.shape[0]
    most_pages = -(-MOSTT // page_rows)
    half = chain // 2
    assert chain & (chain - 1) == 0 and most_pages <= half
    masks = tuple(range(0, half, 2))
    rows = steps * SHARE

    def swap(x, mask):
        return lax.ppermute(x, "seq", [(i, i ^ mask) for i in range(chain)])

    meta = jnp.concatenate([lax.axis_index("seq").reshape(1).astype(jnp.int32), turn_lengths, turn_slot])

    own = (turn_keys.reshape(laps, page_rows, width), turn_values.reshape(laps, page_rows, width))
    got = tuple(swap(x, half) for x in own)
    twin = tuple(swap(x, 1) for x in own)
    got_twin = tuple(swap(x, 1) for x in got)

    q = queries.reshape(steps, slots, KVH, SHARE, HD).transpose(1, 2, 0, 3, 4)
    q = q.reshape(slots, KVH * rows, HD)
    pad = ((0, 0), (0, page_rows - steps), (0, 0))
    new_k = jnp.pad(new_keys.transpose(1, 0, 2), pad)
    new_v = jnp.pad(new_values.transpose(1, 0, 2), pad)
    f32_rows = jax.ShapeDtypeStruct((KVH * rows, HD), jnp.float32)
    part_out, q_mine, acc, top, total = pl.pallas_call(
        functools.partial(resident_kernel, turns),
        out_shape=(
            jax.ShapeDtypeStruct(queries.shape, jnp.bfloat16),
            jax.ShapeDtypeStruct((KVH * rows, HD), jnp.bfloat16),
            f32_rows, f32_rows, f32_rows,
        ),
        in_specs=[SMEM] * 3 + [VMEM] * 3 + [ANY] * 2,
        out_specs=(VMEM,) * 5,
        scratch_shapes=[
            pltpu.VMEM((slots, pages + 1, page_rows, width), jnp.bfloat16),
            pltpu.VMEM((slots, pages + 1, page_rows, width), jnp.bfloat16),
            pltpu.VMEM((slots * KVH * rows, HD), jnp.float32),
            pltpu.SemaphoreType.DMA((slots,)),
            pltpu.SemaphoreType.DMA((slots,)),
        ],
        cost_estimate=pl.CostEstimate(
            flops=4 * slots * KVH * rows * pages * page_rows * HD,
            bytes_accessed=2 * pool_keys.size * 2, transcendentals=0,
        ),
        name="resident",
    )(meta, page_table, cached_len, q, new_k, new_v, pool_keys, pool_values)

    piece = jax.ShapeDtypeStruct((2, 2, page_rows, width), jnp.bfloat16)
    picked = pl.pallas_call(
        functools.partial(pick_kernel, turns, chain, slots, masks),
        out_shape=(piece,) * len(masks),
        in_specs=[SMEM] + [VMEM] * 8,
        out_specs=(VMEM,) * len(masks),
        name="pick",
    )(meta, *own, *twin, *got, *got_twin)
    pieces = [picked[0]] + [swap(x, mask) for x, mask in zip(picked[1:], masks[1:])]

    landed = jax.ShapeDtypeStruct((1, most_pages * page_rows, width), jnp.bfloat16)
    return pl.pallas_call(
        functools.partial(land_kernel, turns, chain, masks),
        out_shape=(jax.ShapeDtypeStruct(queries.shape, jnp.bfloat16), landed, landed),
        in_specs=[SMEM] + [VMEM] * (5 + len(masks)),
        out_specs=(VMEM,) * 3,
        scratch_shapes=[
            pltpu.VMEM((most_pages, page_rows, width), jnp.bfloat16),
            pltpu.VMEM((most_pages, page_rows, width), jnp.bfloat16),
            pltpu.VMEM((KVH * rows, HD), jnp.float32),
        ],
        name="land",
    )(meta, part_out, q_mine, acc, top, total, *pieces)


def solution(mesh):
    both = ("groups", "seq")
    in_specs = (
        P(None, both, None),
        P(None, both, None),
        P(None, both, None),
        P(both, None, None),
        P(both, None, None),
        P(both, None),
        P(both),
        P(None, both, None, None),
        P(None, both, None, None),
        P("groups"),
        P("groups"),
    )
    out_specs = (P(None, both, None), P(both, None, None), P(both, None, None))
    return jax.shard_map(
        per_device, mesh=mesh, in_specs=in_specs, out_specs=out_specs, check_vma=False
    )
```

```python
import functools
import math

import jax
import jax.numpy as jnp
from jax import lax
from jax.experimental import pallas as pl
from jax.experimental.pallas import tpu as pltpu
from jax.sharding import PartitionSpec as P

QH = 64
KVH = 8
HD = 128
MOSTT = 80


SHARE = QH // KVH
LOG2_SCALE = math.log2(math.e) / math.sqrt(HD)
VMEM = pl.BlockSpec(memory_space=pltpu.VMEM)
SMEM = pl.BlockSpec(memory_space=pltpu.SMEM)
HBM = pl.BlockSpec(memory_space=pltpu.HBM)
TRANSPOSED = (((1,), (1,)), ((), ()))


def turn_of(lengths, owners, page_rows, slots_here, owner):
    def look(t, carry):
        first, start, count, length, slot = carry
        tokens = lengths[t]
        pages = (tokens + page_rows - 1) // page_rows
        whose = owners[t]
        mine = whose // slots_here == owner
        return (
            first + pages,
            jnp.where(mine, first, start),
            jnp.where(mine, pages, count),
            jnp.where(mine, tokens, length),
            jnp.where(mine, whose % slots_here, slot),
        )

    zero = jnp.int32(0)
    return lax.fori_loop(0, lengths.shape[0], look, (zero, zero, zero, zero, zero))[1:]


def resident_kernel(
    chain, masks, laps,
    place, turn_lengths, turn_slot, table, lengths, q_hbm, new_k_hbm, new_v_hbm, pool_k, pool_v,
    out, q_mine, acc_mine, max_mine, sum_mine, pick_mask, land_mask, bias, mine_mask,
    q, new_k, new_v, k_buf, v_buf, q_all, new_all, s_new, p_new, acc_all, max_all, sum_all, sems,
):
    steps, slots, _ = out.shape
    page_rows = k_buf.shape[1]
    pages = table.shape[1]
    span = pages * page_rows
    rows = steps * SHARE
    half = chain // 2
    pairs = ((q_hbm, q), (new_k_hbm, new_k), (new_v_hbm, new_v), (pool_k, k_buf), (pool_v, v_buf))
    copies = [pltpu.make_async_copy(*pair, sems.at[i]) for i, pair in enumerate(pairs)]
    for copy in copies:
        copy.start()

    me = place[0]
    row = lax.broadcasted_iota(jnp.int32, (page_rows, HD), 0)
    for i, mask in enumerate(masks):
        start, count, _, _ = turn_of(turn_lengths, turn_slot, page_rows, slots, me ^ mask)
        for slot in range(2):
            residue = me ^ slot
            page = start + ((residue - start) & (half - 1))
            for side in range(2):
                for lap in range(laps):
                    wanted = lap * chain + (residue ^ (side * half))
                    hit = (page == wanted) & (page < start + count)
                    pick_mask[((i * 2 + slot) * 2 + side) * laps + lap] = jnp.full(
                        (page_rows, HD), hit.astype(jnp.float32)
                    ).astype(jnp.bfloat16)
    start, count, length, my_slot = turn_of(turn_lengths, turn_slot, page_rows, slots, me)
    for j in range(land_mask.shape[0]):
        kept = (row + j * page_rows < length).astype(jnp.float32)
        for i, mask in enumerate(masks):
            for slot in range(2):
                hit = (((me ^ mask ^ slot) - start) & (half - 1)) == j
                land_mask[j, i * 2 + slot] = (kept * hit.astype(jnp.float32)).astype(jnp.bfloat16)
    token = lax.broadcasted_iota(jnp.int32, bias.shape, 1)
    bias[...] = jnp.where(token < length, 0.0, -jnp.inf)
    mine_mask[...] = (
        lax.broadcasted_iota(jnp.int32, mine_mask.shape, 0) == my_slot
    ).astype(jnp.float32)

    for copy in copies[:3]:
        copy.wait()
    for kv, new in enumerate((new_k, new_v)):
        for t in range(steps):
            for g in range(KVH):
                new_all[kv, pl.ds((t * KVH + g) * slots, slots), :] = new[
                    t, :, pl.ds(g * HD, HD)
                ].astype(jnp.float32)
    for s in range(steps):
        for g in range(KVH):
            for e in range(SHARE):
                tile = q[s, :, pl.ds((g * SHARE + e) * HD, HD)].astype(jnp.float32)
                q_all[pl.ds(g * rows + s * SHARE + e, slots, stride=KVH * rows), :] = tile

    fresh = (steps * KVH * slots, HD)
    block = KVH * rows
    column = lax.broadcasted_iota(jnp.int32, (block, fresh[0]), 1)
    head_row = lax.broadcasted_iota(jnp.int32, (block, fresh[0]), 0)
    column_slot = column % slots
    causal = (column // slots % KVH == head_row // rows) & (
        column // (slots * KVH) <= head_row % rows // SHARE
    )
    new_keys = new_all[0].astype(jnp.bfloat16)
    for r in range(slots):
        part = pl.ds(r * block, block)
        score = lax.dot_general(
            q_all[part, :].astype(jnp.bfloat16), new_keys, TRANSPOSED,
            preferred_element_type=jnp.float32,
        )
        s_new[part, :] = jnp.where(causal & (column_slot == r), score * LOG2_SCALE, -jnp.inf)

    token = lax.broadcasted_iota(jnp.int32, (2 * rows, span), 1)
    none = jnp.zeros((rows, HD), jnp.bfloat16)
    copies[3].wait()
    copies[4].wait()
    for r in range(slots):
        valid = token < lengths[r]
        where = [table[r, c] for c in range(pages)]
        scores = []
        for g in range(0, KVH, 2):
            first = q_all[pl.ds(r * block + g * rows, rows), :].astype(jnp.bfloat16)
            second = q_all[pl.ds(r * block + (g + 1) * rows, rows), :].astype(jnp.bfloat16)
            both = jnp.concatenate(
                [jnp.concatenate([first, none], 1), jnp.concatenate([none, second], 1)]
            )
            keys = jnp.concatenate([k_buf[c, :, pl.ds(g * HD, 2 * HD)] for c in where])
            scores.append(
                lax.dot_general(both, keys, TRANSPOSED, preferred_element_type=jnp.float32)
            )
        for i, g in enumerate(range(0, KVH, 2)):
            part = pl.ds(r * block + g * rows, 2 * rows)
            score = jnp.where(valid, scores[i] * LOG2_SCALE, -jnp.inf)
            late = s_new[part, :]
            top = jnp.maximum(
                jnp.max(score, axis=1, keepdims=True), jnp.max(late, axis=1, keepdims=True)
            )
            prob = jnp.exp2(score - top)
            late = jnp.exp2(late - top)
            total = jnp.sum(prob, axis=1, keepdims=True) + jnp.sum(late, axis=1, keepdims=True)
            max_all[part, :] = jnp.broadcast_to(top, (2 * rows, HD))
            sum_all[part, :] = jnp.broadcast_to(total, (2 * rows, HD))
            p_new[part, :] = late.astype(jnp.bfloat16)
            values = jnp.concatenate([v_buf[c, :, pl.ds(g * HD, 2 * HD)] for c in where])
            acc = jnp.dot(prob.astype(jnp.bfloat16), values, preferred_element_type=jnp.float32)
            acc_all[pl.ds(r * block + g * rows, rows), :] = acc[:rows, :HD]
            acc_all[pl.ds(r * block + (g + 1) * rows, rows), :] = acc[rows:, HD:]
    new_values = new_all[1].astype(jnp.bfloat16)
    for r in range(slots):
        part = pl.ds(r * block, block)
        acc_all[part, :] += jnp.dot(
            p_new[part, :], new_values, preferred_element_type=jnp.float32
        )

    mine = pl.ds(pl.multiple_of(my_slot * block, block), block)
    acc_mine[...] = acc_all[mine, :]
    max_mine[...] = max_all[mine, :]
    sum_mine[...] = sum_all[mine, :]
    for g in range(0, KVH, 2):
        first = q_all[pl.ds(pl.multiple_of(my_slot * block + g * rows, rows), rows), :]
        second = q_all[pl.ds(pl.multiple_of(my_slot * block + (g + 1) * rows, rows), rows), :]
        q_mine[pl.ds(g * rows, rows), pl.ds(0, HD)] = first.astype(jnp.bfloat16)
        q_mine[pl.ds(g * rows, rows), pl.ds(HD, HD)] = none
        q_mine[pl.ds((g + 1) * rows, rows), pl.ds(0, HD)] = none
        q_mine[pl.ds((g + 1) * rows, rows), pl.ds(HD, HD)] = second.astype(jnp.bfloat16)
    acc_all[...] = acc_all[...] / sum_all[...]
    for s in range(steps):
        for g in range(KVH):
            for e in range(SHARE):
                tile = acc_all[pl.ds(g * rows + s * SHARE + e, slots, stride=block), :]
                out[s, :, pl.ds((g * SHARE + e) * HD, HD)] = tile.astype(jnp.bfloat16)


def pick_kernel(laps, masks, pick_mask, *refs):
    own, twin, got, got_twin = (refs[i : i + 2] for i in range(0, 8, 2))
    width = own[0].shape[2]
    for i, out in enumerate(refs[8:]):
        for slot, sides in enumerate(((own, got), (twin, got_twin))):
            hits = [
                pick_mask[((i * 2 + slot) * 2 + side) * laps + lap] > 0
                for side in range(2)
                for lap in range(laps)
            ]
            for kv in range(2):
                for lane in range(0, width, HD):
                    lanes = pl.ds(lane, HD)
                    pages = [sides[side][kv][lap, :, lanes] for side in range(2) for lap in range(laps)]
                    best = jnp.zeros_like(pages[0])
                    for hit, page in zip(hits, pages):
                        best = jnp.where(hit, page, best)
                    out[slot, kv, :, lanes] = best


def land_kernel(
    masks, part_out, q, acc_old, max_old, sum_old, land_mask, bias, mine_mask, *refs
):
    pieces = refs[: len(masks)]
    out, landed_k, landed_v, o_new = refs[len(masks) :]
    steps, slots, _ = out.shape
    pages, _, page_rows, _ = land_mask.shape
    width = landed_k.shape[2]
    span = pages * page_rows
    rows = steps * SHARE
    for j in range(pages):
        hits = [land_mask[j, i] > 0 for i in range(2 * len(masks))]
        for kv, landed in enumerate((landed_k, landed_v)):
            for lane in range(0, width, HD):
                lanes = pl.ds(lane, HD)
                found = jnp.zeros((page_rows, HD), jnp.bfloat16)
                for i, hit in enumerate(hits):
                    found = jnp.where(hit, pieces[i // 2][i % 2, kv, :, lanes], found)
                landed[0, pl.ds(j * page_rows, page_rows), lanes] = found
    for g in range(0, KVH, 2):
        part = pl.ds(g * rows, 2 * rows)
        lanes = pl.ds(g * HD, 2 * HD)
        score = lax.dot_general(
            q[part, :], landed_k[0, :, lanes], TRANSPOSED, preferred_element_type=jnp.float32
        )
        score = score * LOG2_SCALE + bias[:, :span]
        before = max_old[part, :]
        top = jnp.maximum(before, jnp.max(score, axis=1, keepdims=True))
        prob = jnp.exp2(score - top[:, :span])
        shrink = jnp.exp2(before - top)
        total = sum_old[part, :] * shrink + jnp.sum(prob, axis=1, keepdims=True)
        acc = jnp.dot(
            prob.astype(jnp.bfloat16), landed_v[0, :, lanes], preferred_element_type=jnp.float32
        )
        acc = jnp.concatenate([acc[:rows, :HD], acc[rows:, HD:]])
        o_new[part, :] = (acc_old[part, :] * shrink + acc) / total
    mine = mine_mask[...] > 0
    for s in range(steps):
        for g in range(KVH):
            for e in range(SHARE):
                lanes = pl.ds((g * SHARE + e) * HD, HD)
                fresh = o_new[pl.ds(g * rows + s * SHARE + e, 1), :]
                tile = part_out[s, :, lanes].astype(jnp.float32)
                out[s, :, lanes] = jnp.where(mine, fresh, tile).astype(jnp.bfloat16)


def per_device(
    queries, new_keys, new_values, pool_keys, pool_values, page_table, cached_len,
    turn_keys, turn_values, turn_lengths, turn_slot,
):
    chain = lax.axis_size("seq")
    steps, slots, query_width = queries.shape
    page_rows, width = pool_keys.shape[1:]
    pages = page_table.shape[1]
    laps = turn_keys.shape[0]
    most_pages = -(-MOSTT // page_rows)
    half = chain // 2
    assert chain & (chain - 1) == 0 and most_pages <= half
    masks = tuple(range(0, half, 2))
    rows = steps * SHARE

    def swap(x, mask):
        return lax.ppermute(x, "seq", [(i, i ^ mask) for i in range(chain)])

    place = lax.axis_index("seq").reshape(1).astype(jnp.int32)

    own = (turn_keys.reshape(laps, page_rows, width), turn_values.reshape(laps, page_rows, width))
    got = tuple(swap(x, half) for x in own)
    twin = tuple(swap(x, 1) for x in own)

    f32, bf16 = jnp.float32, jnp.bfloat16
    block = KVH * rows
    stats = jax.ShapeDtypeStruct((block, HD), f32)
    all_rows = pltpu.VMEM((slots * block, HD), f32)
    fresh = (steps * KVH * slots, HD)
    large = tuple(
        pltpu.with_memory_space_constraint(x, pltpu.HBM)
        for x in (queries, new_keys, new_values, pool_keys, pool_values)
    )
    part_out, q_mine, acc, top, total, pick_mask, land_mask, bias, mine_mask = pl.pallas_call(
        functools.partial(resident_kernel, chain, masks, laps),
        out_shape=(
            jax.ShapeDtypeStruct(queries.shape, bf16),
            jax.ShapeDtypeStruct((block, 2 * HD), bf16),
            stats, stats, stats,
            jax.ShapeDtypeStruct((len(masks) * 4 * laps, page_rows, HD), bf16),
            jax.ShapeDtypeStruct((most_pages, 2 * len(masks), page_rows, HD), bf16),
            jax.ShapeDtypeStruct((2 * rows, HD), f32),
            jax.ShapeDtypeStruct((slots, HD), f32),
        ),
        in_specs=[SMEM] * 5 + [HBM] * 5,
        out_specs=(VMEM,) * 9,
        scratch_shapes=[
            *(pltpu.VMEM(x.shape, bf16) for x in large),
            all_rows,
            pltpu.VMEM((2, *fresh), f32),
            all_rows,
            pltpu.VMEM((slots * block, HD), bf16),
            all_rows, all_rows, all_rows,
            pltpu.SemaphoreType.DMA((5,)),
        ],
        compiler_params=pltpu.CompilerParams(vmem_limit_bytes=16 * 2**20),
        cost_estimate=pl.CostEstimate(
            flops=4 * slots * block * pages * page_rows * HD,
            bytes_accessed=2 * pool_keys.size * 2, transcendentals=0,
        ),
        name="resident",
    )(place, turn_lengths, turn_slot, page_table, cached_len, *large)

    *got, part_out = lax.optimization_barrier((*got, part_out))
    got_twin = tuple(swap(x, 1) for x in got)

    piece = jax.ShapeDtypeStruct((2, 2, page_rows, width), bf16)
    picked = pl.pallas_call(
        functools.partial(pick_kernel, laps, masks),
        out_shape=(piece,) * len(masks),
        in_specs=[VMEM] * 9,
        out_specs=(VMEM,) * len(masks),
        compiler_params=pltpu.CompilerParams(vmem_limit_bytes=8 * 2**20),
        name="pick",
    )(pick_mask, *own, *twin, *got, *got_twin)
    pieces = [picked[0]] + [swap(x, mask) for x, mask in zip(picked[1:], masks[1:])]

    landed = jax.ShapeDtypeStruct((1, most_pages * page_rows, width), bf16)
    return pl.pallas_call(
        functools.partial(land_kernel, masks),
        out_shape=(jax.ShapeDtypeStruct(queries.shape, bf16), landed, landed),
        in_specs=[VMEM] * (8 + len(masks)),
        out_specs=(VMEM,) * 3,
        scratch_shapes=[pltpu.VMEM((block, HD), f32)],
        compiler_params=pltpu.CompilerParams(vmem_limit_bytes=8 * 2**20),
        name="land",
    )(part_out, q_mine, acc, top, total, land_mask, bias, mine_mask, *pieces)


def solution(mesh):
    both = ("groups", "seq")
    in_specs = (
        P(None, both, None),
        P(None, both, None),
        P(None, both, None),
        P(both, None, None),
        P(both, None, None),
        P(both, None),
        P(both),
        P(None, both, None, None),
        P(None, both, None, None),
        P("groups"),
        P("groups"),
    )
    out_specs = (P(None, both, None), P(both, None, None), P(both, None, None))
    return jax.shard_map(
        per_device, mesh=mesh, in_specs=in_specs, out_specs=out_specs, check_vma=False
    )
```

```python
import functools
import math

import jax
import jax.numpy as jnp
from jax import lax
from jax.experimental import pallas as pl
from jax.experimental.pallas import tpu as pltpu
from jax.sharding import PartitionSpec as P


QH = 64
KVH = 8
HD = 128
MOSTT = 80


SHARE = QH // KVH
LOG2_SCALE = math.log2(math.e) / math.sqrt(HD)
VMEM = pl.BlockSpec(memory_space=pltpu.VMEM)
SMEM = pl.BlockSpec(memory_space=pltpu.SMEM)
HBM = pl.BlockSpec(memory_space=pltpu.HBM)
TRANSPOSED = (((1,), (1,)), ((), ()))


def turn_of(lengths, owners, page_rows, slots_here, owner):
    def look(t, carry):
        first, start, count, length, slot = carry
        tokens = lengths[t]
        pages = (tokens + page_rows - 1) // page_rows
        whose = owners[t]
        mine = whose // slots_here == owner
        return (
            first + pages,
            jnp.where(mine, first, start),
            jnp.where(mine, pages, count),
            jnp.where(mine, tokens, length),
            jnp.where(mine, whose % slots_here, slot),
        )

    zero = jnp.int32(0)
    return lax.fori_loop(0, lengths.shape[0], look, (zero, zero, zero, zero, zero))[1:]


def prepare_kernel(
    chain, masks, laps, ints,
    place, *refs,
):
    ints_hbm, refs = refs[:ints], refs[ints:]
    q_hbm, new_k_hbm, new_v_hbm, pool_k, pool_v = refs[:5]
    q_all, new_all, k_buf, v_buf, pick_mask, land_mask, bias, mine_mask = refs[5:13]
    q, new_k, new_v = refs[13:16]
    turn_lengths, turn_slot = refs[16 : 16 + ints]
    sems = refs[16 + ints]
    steps, slots, _ = q.shape
    page_rows = k_buf.shape[1]
    rows = steps * SHARE
    half = chain // 2
    pairs = (
        (ints_hbm[0], turn_lengths), (ints_hbm[1], turn_slot),
        (q_hbm, q), (new_k_hbm, new_k), (new_v_hbm, new_v), (pool_k, k_buf), (pool_v, v_buf),
    )
    copies = [pltpu.make_async_copy(*pair, sems.at[i]) for i, pair in enumerate(pairs)]
    for copy in copies:
        copy.start()
    for copy in copies[:2]:
        copy.wait()

    me = place[0]
    row = lax.broadcasted_iota(jnp.int32, (page_rows, HD), 0)
    for i, mask in enumerate(masks):
        start, count, _, _ = turn_of(turn_lengths, turn_slot, page_rows, slots, me ^ mask)
        for slot in range(2):
            residue = me ^ slot
            page = start + ((residue - start) & (half - 1))
            for side in range(2):
                for lap in range(laps):
                    wanted = lap * chain + (residue ^ (side * half))
                    hit = (page == wanted) & (page < start + count)
                    pick_mask[((i * 2 + slot) * 2 + side) * laps + lap] = jnp.full(
                        (page_rows, HD), hit.astype(jnp.float32)
                    ).astype(jnp.bfloat16)
    start, count, length, my_slot = turn_of(turn_lengths, turn_slot, page_rows, slots, me)
    for j in range(land_mask.shape[0]):
        kept = (row + j * page_rows < length).astype(jnp.float32)
        for i, mask in enumerate(masks):
            for slot in range(2):
                hit = (((me ^ mask ^ slot) - start) & (half - 1)) == j
                land_mask[j, i * 2 + slot] = (kept * hit.astype(jnp.float32)).astype(jnp.bfloat16)
    token = lax.broadcasted_iota(jnp.int32, bias.shape, 1)
    bias[...] = jnp.where(token < length, 0.0, -jnp.inf)
    mine_mask[...] = (
        lax.broadcasted_iota(jnp.int32, mine_mask.shape, 0) == my_slot
    ).astype(jnp.float32)

    for copy in copies[2:5]:
        copy.wait()
    for kv, new in enumerate((new_k, new_v)):
        for t in range(steps):
            for g in range(KVH):
                new_all[kv, pl.ds((t * KVH + g) * slots, slots), :] = new[
                    t, :, pl.ds(g * HD, HD)
                ].astype(jnp.float32)
    for s in range(steps):
        for g in range(KVH):
            for e in range(SHARE):
                tile = q[s, :, pl.ds((g * SHARE + e) * HD, HD)].astype(jnp.float32)
                q_all[pl.ds(g * rows + s * SHARE + e, slots, stride=KVH * rows), :] = tile
    for copy in copies[5:]:
        copy.wait()


def resident_kernel(
    place, turn_lengths_hbm, turn_slot_hbm, table_hbm, lengths_hbm, q_all, new_all, k_buf, v_buf,
    out, q_mine, acc_mine, max_mine, sum_mine,
    turn_lengths, turn_slot, table, lengths, s_new, p_new, acc_all, max_all, sum_all, sems,
):
    steps, slots, _ = out.shape
    page_rows = k_buf.shape[1]
    pages = table.shape[1]
    span = pages * page_rows
    rows = steps * SHARE
    pairs = (
        (turn_lengths_hbm, turn_lengths), (turn_slot_hbm, turn_slot),
        (table_hbm, table), (lengths_hbm, lengths),
    )
    copies = [pltpu.make_async_copy(*pair, sems.at[i]) for i, pair in enumerate(pairs)]
    for copy in copies:
        copy.start()

    fresh = (steps * KVH * slots, HD)
    block = KVH * rows
    column = lax.broadcasted_iota(jnp.int32, (block, fresh[0]), 1)
    head_row = lax.broadcasted_iota(jnp.int32, (block, fresh[0]), 0)
    column_slot = column % slots
    causal = (column // slots % KVH == head_row // rows) & (
        column // (slots * KVH) <= head_row % rows // SHARE
    )
    new_keys = new_all[0].astype(jnp.bfloat16)
    for r in range(slots):
        part = pl.ds(r * block, block)
        score = lax.dot_general(
            q_all[part, :].astype(jnp.bfloat16), new_keys, TRANSPOSED,
            preferred_element_type=jnp.float32,
        )
        s_new[part, :] = jnp.where(causal & (column_slot == r), score * LOG2_SCALE, -jnp.inf)

    token = lax.broadcasted_iota(jnp.int32, (2 * rows, span), 1)
    none = jnp.zeros((rows, HD), jnp.bfloat16)
    for copy in copies:
        copy.wait()
    my_slot = turn_of(turn_lengths, turn_slot, page_rows, slots, place[0])[3]
    for r in range(slots):
        valid = token < lengths[r]
        where = [table[r, c] for c in range(pages)]
        scores = []
        for g in range(0, KVH, 2):
            first = q_all[pl.ds(r * block + g * rows, rows), :].astype(jnp.bfloat16)
            second = q_all[pl.ds(r * block + (g + 1) * rows, rows), :].astype(jnp.bfloat16)
            both = jnp.concatenate(
                [jnp.concatenate([first, none], 1), jnp.concatenate([none, second], 1)]
            )
            keys = jnp.concatenate([k_buf[c, :, pl.ds(g * HD, 2 * HD)] for c in where])
            scores.append(
                lax.dot_general(both, keys, TRANSPOSED, preferred_element_type=jnp.float32)
            )
        for i, g in enumerate(range(0, KVH, 2)):
            part = pl.ds(r * block + g * rows, 2 * rows)
            score = jnp.where(valid, scores[i] * LOG2_SCALE, -jnp.inf)
            late = s_new[part, :]
            top = jnp.maximum(
                jnp.max(score, axis=1, keepdims=True), jnp.max(late, axis=1, keepdims=True)
            )
            prob = jnp.exp2(score - top)
            late = jnp.exp2(late - top)
            total = jnp.sum(prob, axis=1, keepdims=True) + jnp.sum(late, axis=1, keepdims=True)
            max_all[part, :] = jnp.broadcast_to(top, (2 * rows, HD))
            sum_all[part, :] = jnp.broadcast_to(total, (2 * rows, HD))
            p_new[part, :] = late.astype(jnp.bfloat16)
            values = jnp.concatenate([v_buf[c, :, pl.ds(g * HD, 2 * HD)] for c in where])
            acc = jnp.dot(prob.astype(jnp.bfloat16), values, preferred_element_type=jnp.float32)
            acc_all[pl.ds(r * block + g * rows, rows), :] = acc[:rows, :HD]
            acc_all[pl.ds(r * block + (g + 1) * rows, rows), :] = acc[rows:, HD:]
    new_values = new_all[1].astype(jnp.bfloat16)
    for r in range(slots):
        part = pl.ds(r * block, block)
        acc_all[part, :] += jnp.dot(
            p_new[part, :], new_values, preferred_element_type=jnp.float32
        )

    mine = pl.ds(pl.multiple_of(my_slot * block, block), block)
    acc_mine[...] = acc_all[mine, :]
    max_mine[...] = max_all[mine, :]
    sum_mine[...] = sum_all[mine, :]
    for g in range(0, KVH, 2):
        first = q_all[pl.ds(pl.multiple_of(my_slot * block + g * rows, rows), rows), :]
        second = q_all[pl.ds(pl.multiple_of(my_slot * block + (g + 1) * rows, rows), rows), :]
        q_mine[pl.ds(g * rows, rows), pl.ds(0, HD)] = first.astype(jnp.bfloat16)
        q_mine[pl.ds(g * rows, rows), pl.ds(HD, HD)] = none
        q_mine[pl.ds((g + 1) * rows, rows), pl.ds(0, HD)] = none
        q_mine[pl.ds((g + 1) * rows, rows), pl.ds(HD, HD)] = second.astype(jnp.bfloat16)
    acc_all[...] = acc_all[...] / sum_all[...]
    for s in range(steps):
        for g in range(KVH):
            for e in range(SHARE):
                tile = acc_all[pl.ds(g * rows + s * SHARE + e, slots, stride=block), :]
                out[s, :, pl.ds((g * SHARE + e) * HD, HD)] = tile.astype(jnp.bfloat16)


def pick_kernel(laps, pick_mask, own, twin, got, got_twin, *outs):
    width = own.shape[2]
    for i, out in enumerate(outs):
        for slot, sides in enumerate(((own, got), (twin, got_twin))):
            hits = [
                pick_mask[((i * 2 + slot) * 2 + side) * laps + lap] > 0
                for side in range(2)
                for lap in range(laps)
            ]
            for lane in range(0, width, HD):
                lanes = pl.ds(lane, HD)
                pages = [sides[side][lap, :, lanes] for side in range(2) for lap in range(laps)]
                best = jnp.zeros_like(pages[0])
                for hit, page in zip(hits, pages):
                    best = jnp.where(hit, page, best)
                out[slot, :, lanes] = best


def land_kernel(
    masks, part_out, q, acc_old, max_old, sum_old, land_mask, bias, mine_mask, *refs
):
    pieces = refs[: len(masks)], refs[len(masks) : 2 * len(masks)]
    out, landed_k, landed_v, o_new = refs[2 * len(masks) :]
    steps, _, _ = out.shape
    pages, _, page_rows, _ = land_mask.shape
    width = landed_k.shape[2]
    span = pages * page_rows
    rows = steps * SHARE
    for j in range(pages):
        hits = [land_mask[j, i] > 0 for i in range(2 * len(masks))]
        for kv, landed in enumerate((landed_k, landed_v)):
            for lane in range(0, width, HD):
                lanes = pl.ds(lane, HD)
                found = jnp.zeros((page_rows, HD), jnp.bfloat16)
                for i, hit in enumerate(hits):
                    found = jnp.where(hit, pieces[kv][i // 2][i % 2, :, lanes], found)
                landed[0, pl.ds(j * page_rows, page_rows), lanes] = found
    for g in range(0, KVH, 2):
        part = pl.ds(g * rows, 2 * rows)
        lanes = pl.ds(g * HD, 2 * HD)
        score = lax.dot_general(
            q[part, :], landed_k[0, :, lanes], TRANSPOSED, preferred_element_type=jnp.float32
        )
        score = score * LOG2_SCALE + bias[:, :span]
        before = max_old[part, :]
        top = jnp.maximum(before, jnp.max(score, axis=1, keepdims=True))
        prob = jnp.exp2(score - top[:, :span])
        shrink = jnp.exp2(before - top)
        total = sum_old[part, :] * shrink + jnp.sum(prob, axis=1, keepdims=True)
        acc = jnp.dot(
            prob.astype(jnp.bfloat16), landed_v[0, :, lanes], preferred_element_type=jnp.float32
        )
        acc = jnp.concatenate([acc[:rows, :HD], acc[rows:, HD:]])
        o_new[part, :] = (acc_old[part, :] * shrink + acc) / total
    mine = mine_mask[...] > 0
    for s in range(steps):
        for g in range(KVH):
            for e in range(SHARE):
                lanes = pl.ds((g * SHARE + e) * HD, HD)
                fresh = o_new[pl.ds(g * rows + s * SHARE + e, 1), :]
                tile = part_out[s, :, lanes].astype(jnp.float32)
                out[s, :, lanes] = jnp.where(mine, fresh, tile).astype(jnp.bfloat16)


def per_device(
    queries, new_keys, new_values, pool_keys, pool_values, page_table, cached_len,
    turn_keys, turn_values, turn_lengths, turn_slot,
):
    chain = lax.axis_size("seq")
    steps, slots, _ = queries.shape
    page_rows, width = pool_keys.shape[1:]
    pages = page_table.shape[1]
    laps = turn_keys.shape[0]
    most_pages = -(-MOSTT // page_rows)
    half = chain // 2
    assert chain & (chain - 1) == 0 and most_pages <= half
    masks = tuple(range(0, half, 2))
    rows = steps * SHARE

    def swap(x, mask):
        return lax.ppermute(x, "seq", [(i, i ^ mask) for i in range(chain)])

    def kernel(body, **settings):
        def call(*args):
            return pl.pallas_call(body, **settings)(*args)

        return call

    place = lax.axis_index("seq").reshape(1).astype(jnp.int32)

    f32, bf16 = jnp.float32, jnp.bfloat16
    block = KVH * rows
    stats = jax.ShapeDtypeStruct((block, HD), f32)
    all_rows = pltpu.VMEM((slots * block, HD), f32)
    fresh = (steps * KVH * slots, HD)
    own_k = turn_keys.reshape(laps, page_rows, width)
    own_v = turn_values.reshape(laps, page_rows, width)

    def in_hbm(*arrays):
        return tuple(pltpu.with_memory_space_constraint(x, pltpu.HBM) for x in arrays)

    got_k = swap(own_k, half)
    twin_k, twin_v = swap(own_k, 1), swap(own_v, 1)
    large = in_hbm(queries, new_keys, new_values, pool_keys, pool_values)
    ints = in_hbm(turn_lengths, turn_slot)
    more_ints = in_hbm(page_table, cached_len)
    q_all, new_all, k_buf, v_buf, pick_mask, land_mask, bias, mine_mask = kernel(
        functools.partial(prepare_kernel, chain, masks, laps, len(ints)),
        out_shape=(
            jax.ShapeDtypeStruct((slots * block, HD), f32),
            jax.ShapeDtypeStruct((2, *fresh), f32),
            jax.ShapeDtypeStruct(pool_keys.shape, bf16),
            jax.ShapeDtypeStruct(pool_values.shape, bf16),
            jax.ShapeDtypeStruct((len(masks) * 4 * laps, page_rows, HD), bf16),
            jax.ShapeDtypeStruct((most_pages, 2 * len(masks), page_rows, HD), bf16),
            jax.ShapeDtypeStruct((2 * rows, HD), f32),
            jax.ShapeDtypeStruct((slots, HD), f32),
        ),
        in_specs=[SMEM] + [HBM] * 7,
        out_specs=(VMEM,) * 8,
        scratch_shapes=[
            *(pltpu.VMEM(x.shape, bf16) for x in large[:3]),
            *(pltpu.SMEM(x.shape, jnp.int32) for x in ints),
            pltpu.SemaphoreType.DMA((7,)),
        ],
        compiler_params=pltpu.CompilerParams(vmem_limit_bytes=16 * 2**20),
    )(place, *ints, *large)
    own_v, q_all = lax.optimization_barrier((own_v, q_all))
    got_v = swap(own_v, half)
    part_out, q_mine, acc, top, total = kernel(
        resident_kernel,
        out_shape=(
            jax.ShapeDtypeStruct(queries.shape, bf16),
            jax.ShapeDtypeStruct((block, 2 * HD), bf16),
            stats, stats, stats,
        ),
        in_specs=[SMEM] + [HBM] * 4 + [VMEM] * 4,
        out_specs=(VMEM,) * 5,
        scratch_shapes=[
            *(pltpu.SMEM(x.shape, jnp.int32) for x in ints + more_ints),
            all_rows,
            pltpu.VMEM((slots * block, HD), bf16),
            all_rows, all_rows, all_rows,
            pltpu.SemaphoreType.DMA((4,)),
        ],
        compiler_params=pltpu.CompilerParams(vmem_limit_bytes=16 * 2**20),
        cost_estimate=pl.CostEstimate(
            flops=4 * slots * block * pages * page_rows * HD,
            bytes_accessed=2 * pool_keys.size * 2, transcendentals=0,
        ),
    )(place, *ints, *more_ints, q_all, new_all, k_buf, v_buf)

    piece = jax.ShapeDtypeStruct((2, page_rows, width), bf16)

    def spread(own, twin, got):
        picked = kernel(
            functools.partial(pick_kernel, laps),
            out_shape=(piece,) * len(masks),
            in_specs=[VMEM] * 5,
            out_specs=(VMEM,) * len(masks),
            compiler_params=pltpu.CompilerParams(vmem_limit_bytes=8 * 2**20),
        )(pick_mask, own, twin, got, swap(got, 1))
        return [picked[0]] + [swap(x, mask) for x, mask in zip(picked[1:], masks[1:])]

    got_k, part_out = lax.optimization_barrier((got_k, part_out))
    pieces_k = spread(own_k, twin_k, got_k)
    pieces_v = spread(own_v, twin_v, got_v)

    landed = jax.ShapeDtypeStruct((1, most_pages * page_rows, width), bf16)
    return kernel(
        functools.partial(land_kernel, masks),
        out_shape=(jax.ShapeDtypeStruct(queries.shape, bf16), landed, landed),
        in_specs=[VMEM] * (8 + 2 * len(masks)),
        out_specs=(VMEM,) * 3,
        scratch_shapes=[pltpu.VMEM((block, HD), f32)],
        compiler_params=pltpu.CompilerParams(vmem_limit_bytes=8 * 2**20),
    )(part_out, q_mine, acc, top, total, land_mask, bias, mine_mask, *pieces_k, *pieces_v)


def solution(mesh):
    both = ("groups", "seq")
    in_specs = (
        P(None, both, None),
        P(None, both, None),
        P(None, both, None),
        P(both, None, None),
        P(both, None, None),
        P(both, None),
        P(both),
        P(None, both, None, None),
        P(None, both, None, None),
        P("groups"),
        P("groups"),
    )
    out_specs = (P(None, both, None), P(both, None, None), P(both, None, None))
    return jax.shard_map(
        per_device, mesh=mesh, in_specs=in_specs, out_specs=out_specs, check_vma=False
    )
```

```python
import functools
import math

import jax
import jax.numpy as jnp
from jax import lax
from jax.experimental import pallas as pl
from jax.experimental.pallas import tpu as pltpu
from jax.sharding import PartitionSpec as P


QH = 64
KVH = 8
HD = 128
MOSTT = 80


SHARE = QH // KVH
LOG2_SCALE = math.log2(math.e) / math.sqrt(HD)
VMEM = pl.BlockSpec(memory_space=pltpu.VMEM)
SMEM = pl.BlockSpec(memory_space=pltpu.SMEM)
HBM = pl.BlockSpec(memory_space=pltpu.HBM)
TRANSPOSED = (((1,), (1,)), ((), ()))


def turn_of(lengths, owners, page_rows, slots_here, owner):
    def look(t, carry):
        first, start, count, length, slot = carry
        tokens = lengths[t]
        pages = (tokens + page_rows - 1) // page_rows
        whose = owners[t]
        mine = whose // slots_here == owner
        return (
            first + pages,
            jnp.where(mine, first, start),
            jnp.where(mine, pages, count),
            jnp.where(mine, tokens, length),
            jnp.where(mine, whose % slots_here, slot),
        )

    zero = jnp.int32(0)
    return lax.fori_loop(0, lengths.shape[0], look, (zero, zero, zero, zero, zero))[1:]


def prepare_kernel(
    chain, masks, laps, ints,
    place, *refs,
):
    ints_hbm, refs = refs[:ints], refs[ints:]
    q_hbm, new_k_hbm, new_v_hbm, pool_k, pool_v = refs[:5]
    q_all, new_all, k_buf, v_buf, pick_mask, land_mask, bias, mine_mask = refs[5:13]
    q, new_k, new_v = refs[13:16]
    turn_lengths, turn_slot = refs[16 : 16 + ints]
    sems = refs[16 + ints]
    steps, slots, _ = q.shape
    page_rows = k_buf.shape[1]
    rows = steps * SHARE
    half = chain // 2
    pairs = (
        (ints_hbm[0], turn_lengths), (ints_hbm[1], turn_slot),
        (q_hbm, q), (new_k_hbm, new_k), (new_v_hbm, new_v), (pool_k, k_buf), (pool_v, v_buf),
    )
    copies = [pltpu.make_async_copy(*pair, sems.at[i]) for i, pair in enumerate(pairs)]
    for copy in copies:
        copy.start()
    for copy in copies[:2]:
        copy.wait()

    me = place[0]
    row = lax.broadcasted_iota(jnp.int32, (page_rows, HD), 0)
    for i, mask in enumerate(masks):
        start, count, _, _ = turn_of(turn_lengths, turn_slot, page_rows, slots, me ^ mask)
        for slot in range(2):
            residue = me ^ slot
            page = start + ((residue - start) & (half - 1))
            for side in range(2):
                for lap in range(laps):
                    wanted = lap * chain + (residue ^ (side * half))
                    hit = (page == wanted) & (page < start + count)
                    pick_mask[((i * 2 + slot) * 2 + side) * laps + lap] = jnp.full(
                        (page_rows, HD), hit.astype(jnp.float32)
                    ).astype(jnp.bfloat16)
    start, count, length, my_slot = turn_of(turn_lengths, turn_slot, page_rows, slots, me)
    for j in range(land_mask.shape[0]):
        kept = (row + j * page_rows < length).astype(jnp.float32)
        for i, mask in enumerate(masks):
            for slot in range(2):
                hit = (((me ^ mask ^ slot) - start) & (half - 1)) == j
                land_mask[j, i * 2 + slot] = (kept * hit.astype(jnp.float32)).astype(jnp.bfloat16)
    token = lax.broadcasted_iota(jnp.int32, bias.shape, 1)
    bias[...] = jnp.where(token < length, 0.0, -jnp.inf)
    mine_mask[...] = (
        lax.broadcasted_iota(jnp.int32, mine_mask.shape, 0) == my_slot
    ).astype(jnp.float32)

    for copy in copies[2:5]:
        copy.wait()
    for kv, new in enumerate((new_k, new_v)):
        for t in range(steps):
            for g in range(KVH):
                new_all[kv, pl.ds((t * KVH + g) * slots, slots), :] = new[
                    t, :, pl.ds(g * HD, HD)
                ].astype(jnp.float32)
    for s in range(steps):
        for g in range(KVH):
            for e in range(SHARE):
                tile = q[s, :, pl.ds((g * SHARE + e) * HD, HD)].astype(jnp.float32)
                q_all[pl.ds(g * rows + s * SHARE + e, slots, stride=KVH * rows), :] = tile
    for copy in copies[5:]:
        copy.wait()


def resident_kernel(
    place, turn_lengths_hbm, turn_slot_hbm, table_hbm, lengths_hbm, q_all, new_all, k_buf, v_buf,
    out, q_mine, acc_mine, max_mine, sum_mine,
    turn_lengths, turn_slot, table, lengths, s_new, p_new, acc_all, max_all, sum_all, sems,
):
    steps, slots, _ = out.shape
    page_rows = k_buf.shape[1]
    pages = table.shape[1]
    span = pages * page_rows
    rows = steps * SHARE
    pairs = (
        (turn_lengths_hbm, turn_lengths), (turn_slot_hbm, turn_slot),
        (table_hbm, table), (lengths_hbm, lengths),
    )
    copies = [pltpu.make_async_copy(*pair, sems.at[i]) for i, pair in enumerate(pairs)]
    for copy in copies:
        copy.start()

    fresh = (steps * KVH * slots, HD)
    block = KVH * rows
    column = lax.broadcasted_iota(jnp.int32, (block, fresh[0]), 1)
    head_row = lax.broadcasted_iota(jnp.int32, (block, fresh[0]), 0)
    column_slot = column % slots
    causal = (column // slots % KVH == head_row // rows) & (
        column // (slots * KVH) <= head_row % rows // SHARE
    )
    new_keys = new_all[0].astype(jnp.bfloat16)
    for r in range(slots):
        part = pl.ds(r * block, block)
        score = lax.dot_general(
            q_all[part, :].astype(jnp.bfloat16), new_keys, TRANSPOSED,
            preferred_element_type=jnp.float32,
        )
        s_new[part, :] = jnp.where(causal & (column_slot == r), score * LOG2_SCALE, -jnp.inf)

    token = lax.broadcasted_iota(jnp.int32, (2 * rows, span), 1)
    none = jnp.zeros((rows, HD), jnp.bfloat16)
    for copy in copies:
        copy.wait()
    my_slot = turn_of(turn_lengths, turn_slot, page_rows, slots, place[0])[3]
    for r in range(slots):
        valid = token < lengths[r]
        where = [table[r, c] for c in range(pages)]
        scores = []
        for g in range(0, KVH, 2):
            first = q_all[pl.ds(r * block + g * rows, rows), :].astype(jnp.bfloat16)
            second = q_all[pl.ds(r * block + (g + 1) * rows, rows), :].astype(jnp.bfloat16)
            both = jnp.concatenate(
                [jnp.concatenate([first, none], 1), jnp.concatenate([none, second], 1)]
            )
            keys = jnp.concatenate([k_buf[c, :, pl.ds(g * HD, 2 * HD)] for c in where])
            scores.append(
                lax.dot_general(both, keys, TRANSPOSED, preferred_element_type=jnp.float32)
            )
        for i, g in enumerate(range(0, KVH, 2)):
            part = pl.ds(r * block + g * rows, 2 * rows)
            score = jnp.where(valid, scores[i] * LOG2_SCALE, -jnp.inf)
            late = s_new[part, :]
            top = jnp.maximum(
                jnp.max(score, axis=1, keepdims=True), jnp.max(late, axis=1, keepdims=True)
            )
            prob = jnp.exp2(score - top)
            late = jnp.exp2(late - top)
            total = jnp.sum(prob, axis=1, keepdims=True) + jnp.sum(late, axis=1, keepdims=True)
            max_all[part, :] = jnp.broadcast_to(top, (2 * rows, HD))
            sum_all[part, :] = jnp.broadcast_to(total, (2 * rows, HD))
            p_new[part, :] = late.astype(jnp.bfloat16)
            values = jnp.concatenate([v_buf[c, :, pl.ds(g * HD, 2 * HD)] for c in where])
            acc = jnp.dot(prob.astype(jnp.bfloat16), values, preferred_element_type=jnp.float32)
            acc_all[pl.ds(r * block + g * rows, rows), :] = acc[:rows, :HD]
            acc_all[pl.ds(r * block + (g + 1) * rows, rows), :] = acc[rows:, HD:]
    new_values = new_all[1].astype(jnp.bfloat16)
    for r in range(slots):
        part = pl.ds(r * block, block)
        acc_all[part, :] += jnp.dot(
            p_new[part, :], new_values, preferred_element_type=jnp.float32
        )

    mine = pl.ds(pl.multiple_of(my_slot * block, block), block)
    acc_mine[...] = acc_all[mine, :]
    max_mine[...] = max_all[mine, :]
    sum_mine[...] = sum_all[mine, :]
    for g in range(0, KVH, 2):
        first = q_all[pl.ds(pl.multiple_of(my_slot * block + g * rows, rows), rows), :]
        second = q_all[pl.ds(pl.multiple_of(my_slot * block + (g + 1) * rows, rows), rows), :]
        q_mine[pl.ds(g * rows, rows), pl.ds(0, HD)] = first.astype(jnp.bfloat16)
        q_mine[pl.ds(g * rows, rows), pl.ds(HD, HD)] = none
        q_mine[pl.ds((g + 1) * rows, rows), pl.ds(0, HD)] = none
        q_mine[pl.ds((g + 1) * rows, rows), pl.ds(HD, HD)] = second.astype(jnp.bfloat16)
    acc_all[...] = acc_all[...] / sum_all[...]
    for s in range(steps):
        for g in range(KVH):
            for e in range(SHARE):
                tile = acc_all[pl.ds(g * rows + s * SHARE + e, slots, stride=block), :]
                out[s, :, pl.ds((g * SHARE + e) * HD, HD)] = tile.astype(jnp.bfloat16)


def pick_kernel(laps, pick_mask, own, twin, got, got_twin, *outs):
    width = own.shape[2]
    for i, out in enumerate(outs):
        for slot, sides in enumerate(((own, got), (twin, got_twin))):
            hits = [
                pick_mask[((i * 2 + slot) * 2 + side) * laps + lap] > 0
                for side in range(2)
                for lap in range(laps)
            ]
            for lane in range(0, width, HD):
                lanes = pl.ds(lane, HD)
                pages = [sides[side][lap, :, lanes] for side in range(2) for lap in range(laps)]
                best = jnp.zeros_like(pages[0])
                for hit, page in zip(hits, pages):
                    best = jnp.where(hit, page, best)
                out[slot, :, lanes] = best


def place_pages(land_mask, pieces, landed):
    pages, _, page_rows, _ = land_mask.shape
    for j in range(pages):
        hits = [land_mask[j, i] > 0 for i in range(2 * len(pieces))]
        for lane in range(0, landed.shape[1], HD):
            lanes = pl.ds(lane, HD)
            found = jnp.zeros((page_rows, HD), jnp.bfloat16)
            for i, hit in enumerate(hits):
                found = jnp.where(hit, pieces[i // 2][i % 2, :, lanes], found)
            landed[pl.ds(j * page_rows, page_rows), lanes] = found


def land_keys_kernel(masks, q, acc_old, max_old, sum_old, land_mask, bias, *refs):
    pieces = refs[: len(masks)]
    landed, weights, base = refs[len(masks) :]
    place_pages(land_mask, pieces, landed)
    rows = q.shape[0] // KVH
    span = landed.shape[0]
    for g in range(0, KVH, 2):
        part = pl.ds(g * rows, 2 * rows)
        score = lax.dot_general(
            q[part, :], landed[:, pl.ds(g * HD, 2 * HD)], TRANSPOSED,
            preferred_element_type=jnp.float32,
        )
        score = score * LOG2_SCALE + bias[:, :span]
        before = max_old[part, :]
        top = jnp.maximum(before, jnp.max(score, axis=1, keepdims=True))
        prob = jnp.exp2(score - top[:, :span])
        shrink = jnp.exp2(before - top)
        total = sum_old[part, :] * shrink + jnp.sum(prob, axis=1, keepdims=True)
        weights[part, :] = (prob / total[:, :span]).astype(jnp.bfloat16)
        base[part, :] = acc_old[part, :] * shrink / total


def land_values_kernel(masks, part_out, weights, base, land_mask, mine_mask, *refs):
    pieces = refs[: len(masks)]
    out_hbm, landed_hbm, out, landed, o_new, sems = refs[len(masks) :]
    steps = out.shape[0]
    rows = steps * SHARE
    place_pages(land_mask, pieces, landed)
    copies = [pltpu.make_async_copy(landed, landed_hbm, sems.at[steps])]
    copies[0].start()
    for g in range(0, KVH, 2):
        acc = jnp.dot(
            weights[pl.ds(g * rows, 2 * rows), :], landed[:, pl.ds(g * HD, 2 * HD)],
            preferred_element_type=jnp.float32,
        )
        first, second = pl.ds(g * rows, rows), pl.ds((g + 1) * rows, rows)
        o_new[first, :] = base[first, :] + acc[:rows, :HD]
        o_new[second, :] = base[second, :] + acc[rows:, HD:]
    mine = mine_mask[...] > 0
    for s in range(steps):
        for g in range(KVH):
            for e in range(SHARE):
                lanes = pl.ds((g * SHARE + e) * HD, HD)
                fresh = o_new[pl.ds(g * rows + s * SHARE + e, 1), :]
                tile = part_out[s, :, lanes].astype(jnp.float32)
                out[s, :, lanes] = jnp.where(mine, fresh, tile).astype(jnp.bfloat16)
        copies.append(pltpu.make_async_copy(out.at[s], out_hbm.at[s], sems.at[s]))
        copies[-1].start()
    for copy in copies:
        copy.wait()


def per_device(
    queries, new_keys, new_values, pool_keys, pool_values, page_table, cached_len,
    turn_keys, turn_values, turn_lengths, turn_slot,
):
    chain = lax.axis_size("seq")
    steps, slots, _ = queries.shape
    page_rows, width = pool_keys.shape[1:]
    pages = page_table.shape[1]
    laps = turn_keys.shape[0]
    most_pages = -(-MOSTT // page_rows)
    half = chain // 2
    assert chain & (chain - 1) == 0 and most_pages <= half
    masks = tuple(range(0, half, 2))
    rows = steps * SHARE

    def swap(x, mask):
        return lax.ppermute(x, "seq", [(i, i ^ mask) for i in range(chain)])

    def kernel(body, **settings):
        def call(*args):
            return pl.pallas_call(body, **settings)(*args)

        return call

    place = lax.axis_index("seq").reshape(1).astype(jnp.int32)

    f32, bf16 = jnp.float32, jnp.bfloat16
    block = KVH * rows
    stats = jax.ShapeDtypeStruct((block, HD), f32)
    all_rows = pltpu.VMEM((slots * block, HD), f32)
    fresh = (steps * KVH * slots, HD)
    own_k = turn_keys.reshape(laps, page_rows, width)
    own_v = turn_values.reshape(laps, page_rows, width)

    def in_hbm(*arrays):
        return tuple(pltpu.with_memory_space_constraint(x, pltpu.HBM) for x in arrays)

    got_k = swap(own_k, half)
    twin_k, twin_v = swap(own_k, 1), swap(own_v, 1)
    large = in_hbm(queries, new_keys, new_values, pool_keys, pool_values)
    ints = in_hbm(turn_lengths, turn_slot)
    more_ints = in_hbm(page_table, cached_len)
    q_all, new_all, k_buf, v_buf, pick_mask, land_mask, bias, mine_mask = kernel(
        functools.partial(prepare_kernel, chain, masks, laps, len(ints)),
        out_shape=(
            jax.ShapeDtypeStruct((slots * block, HD), f32),
            jax.ShapeDtypeStruct((2, *fresh), f32),
            jax.ShapeDtypeStruct(pool_keys.shape, bf16),
            jax.ShapeDtypeStruct(pool_values.shape, bf16),
            jax.ShapeDtypeStruct((len(masks) * 4 * laps, page_rows, HD), bf16),
            jax.ShapeDtypeStruct((most_pages, 2 * len(masks), page_rows, HD), bf16),
            jax.ShapeDtypeStruct((2 * rows, HD), f32),
            jax.ShapeDtypeStruct((slots, HD), f32),
        ),
        in_specs=[SMEM] + [HBM] * 7,
        out_specs=(VMEM,) * 8,
        scratch_shapes=[
            *(pltpu.VMEM(x.shape, bf16) for x in large[:3]),
            *(pltpu.SMEM(x.shape, jnp.int32) for x in ints),
            pltpu.SemaphoreType.DMA((7,)),
        ],
        compiler_params=pltpu.CompilerParams(vmem_limit_bytes=16 * 2**20),
    )(place, *ints, *large)
    own_v, q_all = lax.optimization_barrier((own_v, q_all))
    got_v = swap(own_v, half)
    part_out, q_mine, acc, top, total = kernel(
        resident_kernel,
        out_shape=(
            jax.ShapeDtypeStruct(queries.shape, bf16),
            jax.ShapeDtypeStruct((block, 2 * HD), bf16),
            stats, stats, stats,
        ),
        in_specs=[SMEM] + [HBM] * 4 + [VMEM] * 4,
        out_specs=(VMEM,) * 5,
        scratch_shapes=[
            *(pltpu.SMEM(x.shape, jnp.int32) for x in ints + more_ints),
            all_rows,
            pltpu.VMEM((slots * block, HD), bf16),
            all_rows, all_rows, all_rows,
            pltpu.SemaphoreType.DMA((4,)),
        ],
        compiler_params=pltpu.CompilerParams(vmem_limit_bytes=16 * 2**20),
        cost_estimate=pl.CostEstimate(
            flops=4 * slots * block * pages * page_rows * HD,
            bytes_accessed=2 * pool_keys.size * 2, transcendentals=0,
        ),
    )(place, *ints, *more_ints, q_all, new_all, k_buf, v_buf)

    piece = jax.ShapeDtypeStruct((2, page_rows, width), bf16)

    def spread(own, twin, got):
        picked = kernel(
            functools.partial(pick_kernel, laps),
            out_shape=(piece,) * len(masks),
            in_specs=[VMEM] * 5,
            out_specs=(VMEM,) * len(masks),
            compiler_params=pltpu.CompilerParams(vmem_limit_bytes=8 * 2**20),
        )(pick_mask, own, twin, got, swap(got, 1))
        return [picked[0]] + [swap(x, mask) for x, mask in zip(picked[1:], masks[1:])]

    got_k, part_out = lax.optimization_barrier((got_k, part_out))
    pieces_k = spread(own_k, twin_k, got_k)
    pieces_v = spread(own_v, twin_v, got_v)

    span = most_pages * page_rows
    small = pltpu.CompilerParams(vmem_limit_bytes=8 * 2**20)
    landed_k, weights, base = kernel(
        functools.partial(land_keys_kernel, masks),
        out_shape=(
            jax.ShapeDtypeStruct((span, width), bf16),
            jax.ShapeDtypeStruct((block, span), bf16),
            stats,
        ),
        in_specs=[VMEM] * (6 + len(masks)),
        out_specs=(VMEM,) * 3,
        compiler_params=small,
    )(q_mine, acc, top, total, land_mask, bias, *pieces_k)
    attended, landed_v = kernel(
        functools.partial(land_values_kernel, masks),
        out_shape=(
            jax.ShapeDtypeStruct(queries.shape, bf16), jax.ShapeDtypeStruct((span, width), bf16)
        ),
        in_specs=[VMEM] * (5 + len(masks)),
        out_specs=(HBM, HBM),
        scratch_shapes=[
            pltpu.VMEM(queries.shape, bf16),
            pltpu.VMEM((span, width), bf16),
            pltpu.VMEM((block, HD), f32),
            pltpu.SemaphoreType.DMA((steps + 1,)),
        ],
        compiler_params=small,
    )(part_out, weights, base, land_mask, mine_mask, *pieces_v)
    return attended, landed_k[None], landed_v[None]


def solution(mesh):
    both = ("groups", "seq")
    in_specs = (
        P(None, both, None),
        P(None, both, None),
        P(None, both, None),
        P(both, None, None),
        P(both, None, None),
        P(both, None),
        P(both),
        P(None, both, None, None),
        P(None, both, None, None),
        P("groups"),
        P("groups"),
    )
    out_specs = (P(None, both, None), P(both, None, None), P(both, None, None))
    return jax.shard_map(
        per_device, mesh=mesh, in_specs=in_specs, out_specs=out_specs, check_vma=False
    )
```

```python
import functools
import math

import jax
import jax.numpy as jnp
from jax import lax
from jax.experimental import pallas as pl
from jax.experimental.pallas import tpu as pltpu
from jax.sharding import PartitionSpec as P


QH = 64
KVH = 8
HD = 128
MOSTT = 80


SHARE = QH // KVH
LOG2_SCALE = math.log2(math.e) / math.sqrt(HD)
VMEM = pl.BlockSpec(memory_space=pltpu.VMEM)
SMEM = pl.BlockSpec(memory_space=pltpu.SMEM)
HBM = pl.BlockSpec(memory_space=pltpu.HBM)
TRANSPOSED = (((1,), (1,)), ((), ()))


def turn_of(lengths, owners, page_rows, slots_here, owner):
    def look(t, carry):
        first, start, count, length, slot = carry
        tokens = lengths[t]
        pages = (tokens + page_rows - 1) // page_rows
        whose = owners[t]
        mine = whose // slots_here == owner
        return (
            first + pages,
            jnp.where(mine, first, start),
            jnp.where(mine, pages, count),
            jnp.where(mine, tokens, length),
            jnp.where(mine, whose % slots_here, slot),
        )

    zero = jnp.int32(0)
    return lax.fori_loop(0, lengths.shape[0], look, (zero, zero, zero, zero, zero))[1:]


def prepare_kernel(
    chain, masks, laps, ints,
    place, *refs,
):
    ints_hbm, refs = refs[:ints], refs[ints:]
    q_hbm, new_k_hbm, new_v_hbm, pool_k, pool_v = refs[:5]
    q_all, new_all, s_new, k_buf, v_buf = refs[5:10]
    pick_k, pick_v, land_mask, bias, mine_mask = refs[10:15]
    q, new_k, new_v = refs[15:18]
    turn_lengths, turn_slot = refs[18 : 18 + ints]
    starts, counts, tokens_of, slot_of, sems = refs[18 + ints :]
    steps, slots, _ = q.shape
    page_rows = k_buf.shape[1]
    rows = steps * SHARE
    half = chain // 2
    pairs = (
        (ints_hbm[0], turn_lengths), (ints_hbm[1], turn_slot),
        (q_hbm, q), (new_k_hbm, new_k), (new_v_hbm, new_v), (pool_k, k_buf), (pool_v, v_buf),
    )
    copies = [pltpu.make_async_copy(*pair, sems.at[i]) for i, pair in enumerate(pairs)]
    for copy in copies[:5]:
        copy.start()
    for copy in copies[:2]:
        copy.wait()
    for copy in copies[5:]:
        copy.start()

    me = place[0]

    def note(t, first):
        tokens = turn_lengths[t]
        owner = turn_slot[t] // slots
        counted = (tokens + page_rows - 1) // page_rows
        starts[owner] = first
        counts[owner] = counted
        tokens_of[owner] = tokens
        slot_of[owner] = turn_slot[t] % slots
        return first + counted

    lax.fori_loop(0, turn_lengths.shape[0], note, jnp.int32(0), unroll=4)
    row = lax.broadcasted_iota(jnp.int32, (page_rows, HD), 0)
    for i, mask in enumerate(masks):
        for slot in range(2):
            start, count = starts[me ^ mask ^ slot], counts[me ^ mask ^ slot]
            for pick, residues in ((pick_k, (0,)), (pick_v, (0, 1)[: 2 - 2 * slot])):
                for twin in residues:
                    residue = me ^ twin
                    page = start + ((residue - start) & (half - 1))
                    for side in range(2):
                        for lap in range(laps):
                            wanted = lap * chain + (residue ^ (side * half))
                            hit = (page == wanted) & (page < start + count)
                            line = i * 2 + (slot if pick is pick_k else twin)
                            pick[(line * 2 + side) * laps + lap] = jnp.full(
                                (page_rows, HD), hit.astype(jnp.float32)
                            ).astype(jnp.bfloat16)
    start, length, my_slot = starts[me], tokens_of[me], slot_of[me]
    for j in range(land_mask.shape[0]):
        kept = (row + j * page_rows < length).astype(jnp.float32)
        for i, mask in enumerate(masks):
            for slot in range(2):
                hit = (((me ^ mask ^ slot) - start) & (half - 1)) == j
                land_mask[j, i * 2 + slot] = (kept * hit.astype(jnp.float32)).astype(jnp.bfloat16)
    token = lax.broadcasted_iota(jnp.int32, bias.shape, 1)
    bias[...] = jnp.where(token < length, 0.0, -jnp.inf)
    mine_mask[...] = (
        lax.broadcasted_iota(jnp.int32, mine_mask.shape, 0) == my_slot
    ).astype(jnp.float32)

    for copy in copies[2:5]:
        copy.wait()
    for kv, new in enumerate((new_k, new_v)):
        for t in range(steps):
            for g in range(KVH):
                new_all[kv, pl.ds((t * KVH + g) * slots, slots), :] = new[
                    t, :, pl.ds(g * HD, HD)
                ].astype(jnp.float32)
    for s in range(steps):
        for g in range(KVH):
            for e in range(SHARE):
                tile = q[s, :, pl.ds((g * SHARE + e) * HD, HD)].astype(jnp.float32)
                q_all[pl.ds(g * rows + s * SHARE + e, slots, stride=KVH * rows), :] = tile
    fresh = (steps * KVH * slots, HD)
    block = KVH * rows
    column = lax.broadcasted_iota(jnp.int32, (block, fresh[0]), 1)
    head_row = lax.broadcasted_iota(jnp.int32, (block, fresh[0]), 0)
    column_slot = column % slots
    causal = (column // slots % KVH == head_row // rows) & (
        column // (slots * KVH) <= head_row % rows // SHARE
    )
    new_keys = new_all[0].astype(jnp.bfloat16)
    for r in range(slots):
        part = pl.ds(r * block, block)
        score = lax.dot_general(
            q_all[part, :].astype(jnp.bfloat16), new_keys, TRANSPOSED,
            preferred_element_type=jnp.float32,
        )
        s_new[part, :] = jnp.where(causal & (column_slot == r), score * LOG2_SCALE, -jnp.inf)
    for copy in copies[5:]:
        copy.wait()


def resident_kernel(
    place, turn_lengths_hbm, turn_slot_hbm, table_hbm, lengths_hbm,
    q_all, new_all, s_new, k_buf, v_buf,
    out, q_mine, acc_mine, max_mine, sum_mine,
    turn_lengths, turn_slot, table, lengths, p_new, acc_all, max_all, sum_all, sems,
):
    steps, slots, _ = out.shape
    page_rows = k_buf.shape[1]
    pages = table.shape[1]
    span = pages * page_rows
    rows = steps * SHARE
    block = KVH * rows
    pairs = (
        (turn_lengths_hbm, turn_lengths), (turn_slot_hbm, turn_slot),
        (table_hbm, table), (lengths_hbm, lengths),
    )
    copies = [pltpu.make_async_copy(*pair, sems.at[i]) for i, pair in enumerate(pairs)]
    for copy in copies:
        copy.start()

    token = lax.broadcasted_iota(jnp.int32, (2 * rows, span), 1)
    none = jnp.zeros((rows, HD), jnp.bfloat16)
    for copy in copies:
        copy.wait()
    my_slot = turn_of(turn_lengths, turn_slot, page_rows, slots, place[0])[3]
    for r in range(slots):
        valid = token < lengths[r]
        where = [table[r, c] for c in range(pages)]
        scores = []
        for g in range(0, KVH, 2):
            first = q_all[pl.ds(r * block + g * rows, rows), :].astype(jnp.bfloat16)
            second = q_all[pl.ds(r * block + (g + 1) * rows, rows), :].astype(jnp.bfloat16)
            both = jnp.concatenate(
                [jnp.concatenate([first, none], 1), jnp.concatenate([none, second], 1)]
            )
            keys = jnp.concatenate([k_buf[c, :, pl.ds(g * HD, 2 * HD)] for c in where])
            scores.append(
                lax.dot_general(both, keys, TRANSPOSED, preferred_element_type=jnp.float32)
            )
        for i, g in enumerate(range(0, KVH, 2)):
            part = pl.ds(r * block + g * rows, 2 * rows)
            score = jnp.where(valid, scores[i] * LOG2_SCALE, -jnp.inf)
            late = s_new[part, :]
            top = jnp.maximum(
                jnp.max(score, axis=1, keepdims=True), jnp.max(late, axis=1, keepdims=True)
            )
            prob = jnp.exp2(score - top)
            late = jnp.exp2(late - top)
            total = jnp.sum(prob, axis=1, keepdims=True) + jnp.sum(late, axis=1, keepdims=True)
            max_all[part, :] = jnp.broadcast_to(top, (2 * rows, HD))
            sum_all[part, :] = jnp.broadcast_to(total, (2 * rows, HD))
            p_new[part, :] = late.astype(jnp.bfloat16)
            values = jnp.concatenate([v_buf[c, :, pl.ds(g * HD, 2 * HD)] for c in where])
            acc = jnp.dot(prob.astype(jnp.bfloat16), values, preferred_element_type=jnp.float32)
            acc_all[pl.ds(r * block + g * rows, rows), :] = acc[:rows, :HD]
            acc_all[pl.ds(r * block + (g + 1) * rows, rows), :] = acc[rows:, HD:]
    new_values = new_all[1].astype(jnp.bfloat16)
    for r in range(slots):
        part = pl.ds(r * block, block)
        acc_all[part, :] += jnp.dot(
            p_new[part, :], new_values, preferred_element_type=jnp.float32
        )

    mine = pl.ds(pl.multiple_of(my_slot * block, block), block)
    acc_mine[...] = acc_all[mine, :]
    max_mine[...] = max_all[mine, :]
    sum_mine[...] = sum_all[mine, :]
    for g in range(0, KVH, 2):
        first = q_all[pl.ds(pl.multiple_of(my_slot * block + g * rows, rows), rows), :]
        second = q_all[pl.ds(pl.multiple_of(my_slot * block + (g + 1) * rows, rows), rows), :]
        q_mine[pl.ds(g * rows, rows), pl.ds(0, HD)] = first.astype(jnp.bfloat16)
        q_mine[pl.ds(g * rows, rows), pl.ds(HD, HD)] = none
        q_mine[pl.ds((g + 1) * rows, rows), pl.ds(0, HD)] = none
        q_mine[pl.ds((g + 1) * rows, rows), pl.ds(HD, HD)] = second.astype(jnp.bfloat16)
    acc_all[...] = acc_all[...] / sum_all[...]
    for s in range(steps):
        for g in range(KVH):
            for e in range(SHARE):
                tile = acc_all[pl.ds(g * rows + s * SHARE + e, slots, stride=block), :]
                out[s, :, pl.ds((g * SHARE + e) * HD, HD)] = tile.astype(jnp.bfloat16)


def pick_kernel(laps, masks, pick_mask, *refs):
    sources, outs = refs[: -len(masks)], refs[-len(masks) :]
    pairs = [sources[i : i + 2] for i in range(0, len(sources), 2)]
    width = sources[0].shape[2]
    for i, out in enumerate(outs):
        for line in range(2):
            sides = pairs[line % len(pairs)]
            hits = [
                pick_mask[((i * 2 + line) * 2 + side) * laps + lap] > 0
                for side in range(2)
                for lap in range(laps)
            ]
            for lane in range(0, width, HD):
                lanes = pl.ds(lane, HD)
                pages = [sides[side][lap, :, lanes] for side in range(2) for lap in range(laps)]
                best = jnp.zeros_like(pages[0])
                for hit, page in zip(hits, pages):
                    best = jnp.where(hit, page, best)
                out[line, :, lanes] = best


def join_kernel(*refs):
    for i, piece in enumerate(refs[:-1]):
        refs[-1][i] = piece[1]


def place_pages(land_mask, pieces, landed):
    pages, _, page_rows, _ = land_mask.shape
    for j in range(pages):
        hits = [land_mask[j, i] > 0 for i in range(len(pieces))]
        for lane in range(0, landed.shape[1], HD):
            lanes = pl.ds(lane, HD)
            found = jnp.zeros((page_rows, HD), jnp.bfloat16)
            for i, hit in enumerate(hits):
                piece, line = pieces[i]
                found = jnp.where(hit, piece[line, :, lanes], found)
            landed[pl.ds(j * page_rows, page_rows), lanes] = found


def land_keys_kernel(masks, q, acc_old, max_old, sum_old, land_mask, bias, *refs):
    pieces, other = refs[: len(masks)], refs[len(masks)]
    landed, weights, base = refs[len(masks) + 1 :]
    lines = [line for i, piece in enumerate(pieces) for line in ((piece, 0), (other, i))]
    place_pages(land_mask, lines, landed)
    rows = q.shape[0] // KVH
    span = landed.shape[0]
    for g in range(0, KVH, 2):
        part = pl.ds(g * rows, 2 * rows)
        score = lax.dot_general(
            q[part, :], landed[:, pl.ds(g * HD, 2 * HD)], TRANSPOSED,
            preferred_element_type=jnp.float32,
        )
        score = score * LOG2_SCALE + bias[:, :span]
        before = max_old[part, :]
        top = jnp.maximum(before, jnp.max(score, axis=1, keepdims=True))
        prob = jnp.exp2(score - top[:, :span])
        shrink = jnp.exp2(before - top)
        total = sum_old[part, :] * shrink + jnp.sum(prob, axis=1, keepdims=True)
        weights[part, :] = (prob / total[:, :span]).astype(jnp.bfloat16)
        base[part, :] = acc_old[part, :] * shrink / total


def land_values_kernel(masks, part_out, weights, base, land_mask, mine_mask, *refs):
    pieces = refs[: len(masks)]
    out_hbm, landed_hbm, out, landed, o_new, sems = refs[len(masks) :]
    steps = out.shape[0]
    rows = steps * SHARE
    place_pages(land_mask, [(piece, line) for piece in pieces for line in range(2)], landed)
    copies = [pltpu.make_async_copy(landed, landed_hbm, sems.at[steps])]
    copies[0].start()
    for g in range(0, KVH, 2):
        acc = jnp.dot(
            weights[pl.ds(g * rows, 2 * rows), :], landed[:, pl.ds(g * HD, 2 * HD)],
            preferred_element_type=jnp.float32,
        )
        first, second = pl.ds(g * rows, rows), pl.ds((g + 1) * rows, rows)
        o_new[first, :] = base[first, :] + acc[:rows, :HD]
        o_new[second, :] = base[second, :] + acc[rows:, HD:]
    mine = mine_mask[...] > 0
    for s in range(steps):
        for g in range(KVH):
            for e in range(SHARE):
                lanes = pl.ds((g * SHARE + e) * HD, HD)
                fresh = o_new[pl.ds(g * rows + s * SHARE + e, 1), :]
                tile = part_out[s, :, lanes].astype(jnp.float32)
                out[s, :, lanes] = jnp.where(mine, fresh, tile).astype(jnp.bfloat16)
        copies.append(pltpu.make_async_copy(out.at[s], out_hbm.at[s], sems.at[s]))
        copies[-1].start()
    for copy in copies:
        copy.wait()


def per_device(
    queries, new_keys, new_values, pool_keys, pool_values, page_table, cached_len,
    turn_keys, turn_values, turn_lengths, turn_slot,
):
    chain = lax.axis_size("seq")
    steps, slots, _ = queries.shape
    page_rows, width = pool_keys.shape[1:]
    pages = page_table.shape[1]
    laps = turn_keys.shape[0]
    most_pages = -(-MOSTT // page_rows)
    half = chain // 2
    assert chain & (chain - 1) == 0 and most_pages <= half
    masks = tuple(range(0, half, 2))
    rows = steps * SHARE

    def swap(x, mask):
        return lax.ppermute(x, "seq", [(i, i ^ mask) for i in range(chain)])

    def kernel(body, **settings):
        def call(*args):
            return pl.pallas_call(body, **settings)(*args)

        return call

    place = lax.axis_index("seq").reshape(1).astype(jnp.int32)

    f32, bf16 = jnp.float32, jnp.bfloat16
    block = KVH * rows
    stats = jax.ShapeDtypeStruct((block, HD), f32)
    all_rows = pltpu.VMEM((slots * block, HD), f32)
    fresh = (steps * KVH * slots, HD)
    own_k = turn_keys.reshape(laps, page_rows, width)
    own_v = turn_values.reshape(laps, page_rows, width)

    def in_hbm(*arrays):
        return tuple(pltpu.with_memory_space_constraint(x, pltpu.HBM) for x in arrays)

    got_k = swap(own_k, half)
    twin_v = swap(own_v, 1)
    large = in_hbm(queries, new_keys, new_values, pool_keys, pool_values)
    ints = in_hbm(turn_lengths, turn_slot)
    more_ints = in_hbm(page_table, cached_len)
    q_all, new_all, s_new, k_buf, v_buf, *tables = kernel(
        functools.partial(prepare_kernel, chain, masks, laps, len(ints)),
        out_shape=(
            jax.ShapeDtypeStruct((slots * block, HD), f32),
            jax.ShapeDtypeStruct((2, *fresh), f32),
            jax.ShapeDtypeStruct((slots * block, fresh[0]), f32),
            jax.ShapeDtypeStruct(pool_keys.shape, bf16),
            jax.ShapeDtypeStruct(pool_values.shape, bf16),
            jax.ShapeDtypeStruct((len(masks) * 4 * laps, page_rows, HD), bf16),
            jax.ShapeDtypeStruct((len(masks) * 4 * laps, page_rows, HD), bf16),
            jax.ShapeDtypeStruct((most_pages, 2 * len(masks), page_rows, HD), bf16),
            jax.ShapeDtypeStruct((2 * rows, HD), f32),
            jax.ShapeDtypeStruct((slots, HD), f32),
        ),
        in_specs=[SMEM] + [HBM] * 7,
        out_specs=(VMEM,) * 10,
        scratch_shapes=[
            *(pltpu.VMEM(x.shape, bf16) for x in large[:3]),
            *(pltpu.SMEM(x.shape, jnp.int32) for x in ints),
            *(pltpu.SMEM((chain,), jnp.int32) for _ in range(4)),
            pltpu.SemaphoreType.DMA((7,)),
        ],
        compiler_params=pltpu.CompilerParams(vmem_limit_bytes=16 * 2**20),
    )(place, *ints, *large)
    mask_k, mask_v, land_mask, bias, mine_mask = tables
    own_v, q_all = lax.optimization_barrier((own_v, q_all))
    got_v = swap(own_v, half)
    part_out, q_mine, acc, top, total = kernel(
        resident_kernel,
        out_shape=(
            jax.ShapeDtypeStruct(queries.shape, bf16),
            jax.ShapeDtypeStruct((block, 2 * HD), bf16),
            stats, stats, stats,
        ),
        in_specs=[SMEM] + [HBM] * 4 + [VMEM] * 5,
        out_specs=(VMEM,) * 5,
        scratch_shapes=[
            *(pltpu.SMEM(x.shape, jnp.int32) for x in ints + more_ints),
            pltpu.VMEM((slots * block, HD), bf16),
            all_rows, all_rows, all_rows,
            pltpu.SemaphoreType.DMA((4,)),
        ],
        compiler_params=pltpu.CompilerParams(vmem_limit_bytes=16 * 2**20),
        cost_estimate=pl.CostEstimate(
            flops=4 * slots * block * pages * page_rows * HD,
            bytes_accessed=2 * pool_keys.size * 2, transcendentals=0,
        ),
    )(place, *ints, *more_ints, q_all, new_all, s_new, k_buf, v_buf)

    piece = jax.ShapeDtypeStruct((2, page_rows, width), bf16)
    small = pltpu.CompilerParams(vmem_limit_bytes=8 * 2**20)

    def spread(*operands):
        picked = kernel(
            functools.partial(pick_kernel, laps, masks),
            out_shape=(piece,) * len(masks),
            in_specs=[VMEM] * len(operands),
            out_specs=(VMEM,) * len(masks),
            compiler_params=small,
        )(*operands)
        return [picked[0]] + [swap(x, mask) for x, mask in zip(picked[1:], masks[1:])]

    got_k, part_out = lax.optimization_barrier((got_k, part_out))
    pieces_k = spread(mask_k, own_k, got_k)
    pieces_v = spread(mask_v, own_v, got_v, twin_v, swap(got_v, 1))
    joined = kernel(
        join_kernel,
        out_shape=jax.ShapeDtypeStruct((len(masks), page_rows, width), bf16),
        in_specs=[VMEM] * len(masks),
        out_specs=VMEM,
        compiler_params=small,
    )(*pieces_k)
    other_k = swap(joined, 1)

    span = most_pages * page_rows
    landed_k, weights, base = kernel(
        functools.partial(land_keys_kernel, masks),
        out_shape=(
            jax.ShapeDtypeStruct((span, width), bf16),
            jax.ShapeDtypeStruct((block, span), bf16),
            stats,
        ),
        in_specs=[VMEM] * (7 + len(masks)),
        out_specs=(VMEM,) * 3,
        compiler_params=small,
    )(q_mine, acc, top, total, land_mask, bias, *pieces_k, other_k)
    attended, landed_v = kernel(
        functools.partial(land_values_kernel, masks),
        out_shape=(
            jax.ShapeDtypeStruct(queries.shape, bf16), jax.ShapeDtypeStruct((span, width), bf16)
        ),
        in_specs=[VMEM] * (5 + len(masks)),
        out_specs=(HBM, HBM),
        scratch_shapes=[
            pltpu.VMEM(queries.shape, bf16),
            pltpu.VMEM((span, width), bf16),
            pltpu.VMEM((block, HD), f32),
            pltpu.SemaphoreType.DMA((steps + 1,)),
        ],
        compiler_params=small,
    )(part_out, weights, base, land_mask, mine_mask, *pieces_v)
    return attended, landed_k[None], landed_v[None]


def solution(mesh):
    both = ("groups", "seq")
    in_specs = (
        P(None, both, None),
        P(None, both, None),
        P(None, both, None),
        P(both, None, None),
        P(both, None, None),
        P(both, None),
        P(both),
        P(None, both, None, None),
        P(None, both, None, None),
        P("groups"),
        P("groups"),
    )
    out_specs = (P(None, both, None), P(both, None, None), P(both, None, None))
    return jax.shard_map(
        per_device, mesh=mesh, in_specs=in_specs, out_specs=out_specs, check_vma=False
    )
```

```python
import functools
import math

import jax
import jax.numpy as jnp
from jax import lax
from jax.experimental import pallas as pl
from jax.experimental.pallas import tpu as pltpu
from jax.sharding import PartitionSpec as P


QH = 64
KVH = 8
HD = 128
MOSTT = 80


SHARE = QH // KVH
LOG2_SCALE = math.log2(math.e) / math.sqrt(HD)
VMEM = pl.BlockSpec(memory_space=pltpu.VMEM)
SMEM = pl.BlockSpec(memory_space=pltpu.SMEM)
HBM = pl.BlockSpec(memory_space=pltpu.HBM)
TRANSPOSED = (((1,), (1,)), ((), ()))


def turn_of(lengths, owners, page_rows, slots_here, owner):
    def look(t, carry):
        first, start, count, length, slot = carry
        tokens = lengths[t]
        pages = (tokens + page_rows - 1) // page_rows
        whose = owners[t]
        mine = whose // slots_here == owner
        return (
            first + pages,
            jnp.where(mine, first, start),
            jnp.where(mine, pages, count),
            jnp.where(mine, tokens, length),
            jnp.where(mine, whose % slots_here, slot),
        )

    zero = jnp.int32(0)
    return lax.fori_loop(0, lengths.shape[0], look, (zero, zero, zero, zero, zero))[1:]


def prepare_kernel(
    chain, masks, laps, ints,
    place, *refs,
):
    ints_hbm, refs = refs[:ints], refs[ints:]
    q_hbm, new_k_hbm, new_v_hbm, pool_k, pool_v = refs[:5]
    q_all, new_all, s_new, k_buf, v_buf = refs[5:10]
    pick_k, pick_v, land_mask, bias, mine_mask = refs[10:15]
    q, new_k, new_v = refs[15:18]
    turn_lengths, turn_slot = refs[18 : 18 + ints]
    starts, counts, tokens_of, slot_of, sems = refs[18 + ints :]
    steps, slots, _ = q.shape
    page_rows = k_buf.shape[1]
    rows = steps * SHARE
    half = chain // 2
    pairs = (
        (ints_hbm[0], turn_lengths), (ints_hbm[1], turn_slot),
        (q_hbm, q), (new_k_hbm, new_k), (new_v_hbm, new_v), (pool_k, k_buf), (pool_v, v_buf),
    )
    copies = [pltpu.make_async_copy(*pair, sems.at[i]) for i, pair in enumerate(pairs)]
    for copy in copies[:5]:
        copy.start()
    for copy in copies[:2]:
        copy.wait()
    for copy in copies[5:]:
        copy.start()

    me = place[0]

    def note(t, first):
        tokens = turn_lengths[t]
        owner = turn_slot[t] // slots
        counted = (tokens + page_rows - 1) // page_rows
        starts[owner] = first
        counts[owner] = counted
        tokens_of[owner] = tokens
        slot_of[owner] = turn_slot[t] % slots
        return first + counted

    lax.fori_loop(0, turn_lengths.shape[0], note, jnp.int32(0), unroll=4)
    row = lax.broadcasted_iota(jnp.int32, (page_rows, HD), 0)
    for i, mask in enumerate(masks):
        for slot in range(2):
            start, count = starts[me ^ mask ^ slot], counts[me ^ mask ^ slot]
            for pick, residues in ((pick_k, (0,)), (pick_v, (0, 1)[: 2 - 2 * slot])):
                for twin in residues:
                    residue = me ^ twin
                    page = start + ((residue - start) & (half - 1))
                    for side in range(2):
                        for lap in range(laps):
                            wanted = lap * chain + (residue ^ (side * half))
                            hit = (page == wanted) & (page < start + count)
                            line = i * 2 + (slot if pick is pick_k else twin)
                            pick[(line * 2 + side) * laps + lap] = jnp.full(
                                (page_rows, HD), hit.astype(jnp.float32)
                            ).astype(jnp.bfloat16)
    start, length, my_slot = starts[me], tokens_of[me], slot_of[me]
    for j in range(land_mask.shape[0]):
        kept = (row + j * page_rows < length).astype(jnp.float32)
        for i, mask in enumerate(masks):
            for slot in range(2):
                hit = (((me ^ mask ^ slot) - start) & (half - 1)) == j
                land_mask[j, i * 2 + slot] = (kept * hit.astype(jnp.float32)).astype(jnp.bfloat16)
    token = lax.broadcasted_iota(jnp.int32, bias.shape, 1)
    bias[...] = jnp.where(token < length, 0.0, -jnp.inf)
    mine_mask[...] = (
        lax.broadcasted_iota(jnp.int32, mine_mask.shape, 0) == my_slot
    ).astype(jnp.float32)

    for copy in copies[2:5]:
        copy.wait()
    for kv, new in enumerate((new_k, new_v)):
        for t in range(steps):
            for g in range(KVH):
                new_all[kv, pl.ds((t * KVH + g) * slots, slots), :] = new[
                    t, :, pl.ds(g * HD, HD)
                ].astype(jnp.float32)
    for s in range(steps):
        for g in range(KVH):
            for e in range(SHARE):
                tile = q[s, :, pl.ds((g * SHARE + e) * HD, HD)].astype(jnp.float32)
                q_all[pl.ds(g * rows + s * SHARE + e, slots, stride=KVH * rows), :] = tile
    fresh = (steps * KVH * slots, HD)
    block = KVH * rows
    column = lax.broadcasted_iota(jnp.int32, (block, fresh[0]), 1)
    head_row = lax.broadcasted_iota(jnp.int32, (block, fresh[0]), 0)
    column_slot = column % slots
    causal = (column // slots % KVH == head_row // rows) & (
        column // (slots * KVH) <= head_row % rows // SHARE
    )
    new_keys = new_all[0].astype(jnp.bfloat16)
    for r in range(slots):
        part = pl.ds(r * block, block)
        score = lax.dot_general(
            q_all[part, :].astype(jnp.bfloat16), new_keys, TRANSPOSED,
            preferred_element_type=jnp.float32,
        )
        s_new[part, :] = jnp.where(causal & (column_slot == r), score * LOG2_SCALE, -jnp.inf)
    for copy in copies[5:]:
        copy.wait()


def resident_kernel(
    place, turn_lengths_hbm, turn_slot_hbm, table_hbm, lengths_hbm,
    q_all, new_all, s_new, k_buf, v_buf,
    out, q_mine, acc_mine, max_mine, sum_mine,
    turn_lengths, turn_slot, table, lengths, p_new, acc_all, max_all, sum_all, sems,
):
    steps, slots, _ = out.shape
    page_rows = k_buf.shape[1]
    pages = table.shape[1]
    span = pages * page_rows
    rows = steps * SHARE
    block = KVH * rows
    pairs = (
        (turn_lengths_hbm, turn_lengths), (turn_slot_hbm, turn_slot),
        (table_hbm, table), (lengths_hbm, lengths),
    )
    copies = [pltpu.make_async_copy(*pair, sems.at[i]) for i, pair in enumerate(pairs)]
    for copy in copies:
        copy.start()

    token = lax.broadcasted_iota(jnp.int32, (2 * rows, span), 1)
    none = jnp.zeros((rows, HD), jnp.bfloat16)
    for copy in copies:
        copy.wait()
    my_slot = turn_of(turn_lengths, turn_slot, page_rows, slots, place[0])[3]
    for r in range(slots):
        valid = token < lengths[r]
        where = [table[r, c] for c in range(pages)]
        scores = []
        for g in range(0, KVH, 2):
            first = q_all[pl.ds(r * block + g * rows, rows), :].astype(jnp.bfloat16)
            second = q_all[pl.ds(r * block + (g + 1) * rows, rows), :].astype(jnp.bfloat16)
            both = jnp.concatenate(
                [jnp.concatenate([first, none], 1), jnp.concatenate([none, second], 1)]
            )
            keys = jnp.concatenate([k_buf[c, :, pl.ds(g * HD, 2 * HD)] for c in where])
            scores.append(
                lax.dot_general(both, keys, TRANSPOSED, preferred_element_type=jnp.float32)
            )
        for i, g in enumerate(range(0, KVH, 2)):
            part = pl.ds(r * block + g * rows, 2 * rows)
            score = jnp.where(valid, scores[i] * LOG2_SCALE, -jnp.inf)
            late = s_new[part, :]
            top = jnp.maximum(
                jnp.max(score, axis=1, keepdims=True), jnp.max(late, axis=1, keepdims=True)
            )
            prob = jnp.exp2(score - top)
            late = jnp.exp2(late - top)
            total = jnp.sum(prob, axis=1, keepdims=True) + jnp.sum(late, axis=1, keepdims=True)
            max_all[part, :] = jnp.broadcast_to(top, (2 * rows, HD))
            sum_all[part, :] = jnp.broadcast_to(total, (2 * rows, HD))
            p_new[part, :] = late.astype(jnp.bfloat16)
            values = jnp.concatenate([v_buf[c, :, pl.ds(g * HD, 2 * HD)] for c in where])
            acc = jnp.dot(prob.astype(jnp.bfloat16), values, preferred_element_type=jnp.float32)
            acc_all[pl.ds(r * block + g * rows, rows), :] = acc[:rows, :HD]
            acc_all[pl.ds(r * block + (g + 1) * rows, rows), :] = acc[rows:, HD:]
    new_values = new_all[1].astype(jnp.bfloat16)
    for r in range(slots):
        part = pl.ds(r * block, block)
        acc_all[part, :] += jnp.dot(
            p_new[part, :], new_values, preferred_element_type=jnp.float32
        )

    mine = pl.ds(pl.multiple_of(my_slot * block, block), block)
    acc_mine[...] = acc_all[mine, :]
    max_mine[...] = max_all[mine, :]
    sum_mine[...] = sum_all[mine, :]
    for g in range(0, KVH, 2):
        first = q_all[pl.ds(pl.multiple_of(my_slot * block + g * rows, rows), rows), :]
        second = q_all[pl.ds(pl.multiple_of(my_slot * block + (g + 1) * rows, rows), rows), :]
        q_mine[pl.ds(g * rows, rows), pl.ds(0, HD)] = first.astype(jnp.bfloat16)
        q_mine[pl.ds(g * rows, rows), pl.ds(HD, HD)] = none
        q_mine[pl.ds((g + 1) * rows, rows), pl.ds(0, HD)] = none
        q_mine[pl.ds((g + 1) * rows, rows), pl.ds(HD, HD)] = second.astype(jnp.bfloat16)
    acc_all[...] = acc_all[...] / sum_all[...]
    for s in range(steps):
        for g in range(KVH):
            for e in range(SHARE):
                tile = acc_all[pl.ds(g * rows + s * SHARE + e, slots, stride=block), :]
                out[s, :, pl.ds((g * SHARE + e) * HD, HD)] = tile.astype(jnp.bfloat16)


def pick_kernel(laps, places, pick_mask, *refs):
    sources, outs = refs[: -len(places)], refs[-len(places) :]
    pairs = [sources[i : i + 2] for i in range(0, len(sources), 2)]
    width = sources[0].shape[2]
    for i, out in zip(places, outs):
        for line in range(2):
            sides = pairs[line % len(pairs)]
            hits = [
                pick_mask[((i * 2 + line) * 2 + side) * laps + lap] > 0
                for side in range(2)
                for lap in range(laps)
            ]
            for lane in range(0, width, HD):
                lanes = pl.ds(lane, HD)
                pages = [sides[side][lap, :, lanes] for side in range(2) for lap in range(laps)]
                best = jnp.zeros_like(pages[0])
                for hit, page in zip(hits, pages):
                    best = jnp.where(hit, page, best)
                out[line, :, lanes] = best


def join_kernel(*refs):
    for i, piece in enumerate(refs[:-1]):
        refs[-1][i] = piece[1]


def place_pages(land_mask, pieces, landed):
    pages, _, page_rows, _ = land_mask.shape
    for j in range(pages):
        hits = [land_mask[j, i] > 0 for i in range(len(pieces))]
        for lane in range(0, landed.shape[1], HD):
            lanes = pl.ds(lane, HD)
            found = jnp.zeros((page_rows, HD), jnp.bfloat16)
            for i, hit in enumerate(hits):
                piece, line = pieces[i]
                found = jnp.where(hit, piece[line, :, lanes], found)
            landed[pl.ds(j * page_rows, page_rows), lanes] = found


def land_keys_kernel(masks, q, acc_old, max_old, sum_old, land_mask, bias, *refs):
    pieces, other = refs[: len(masks)], refs[len(masks)]
    landed, weights, base = refs[len(masks) + 1 :]
    lines = [line for i, piece in enumerate(pieces) for line in ((piece, 0), (other, i))]
    place_pages(land_mask, lines, landed)
    rows = q.shape[0] // KVH
    span = landed.shape[0]
    for g in range(0, KVH, 2):
        part = pl.ds(g * rows, 2 * rows)
        score = lax.dot_general(
            q[part, :], landed[:, pl.ds(g * HD, 2 * HD)], TRANSPOSED,
            preferred_element_type=jnp.float32,
        )
        score = score * LOG2_SCALE + bias[:, :span]
        before = max_old[part, :]
        top = jnp.maximum(before, jnp.max(score, axis=1, keepdims=True))
        prob = jnp.exp2(score - top[:, :span])
        shrink = jnp.exp2(before - top)
        total = sum_old[part, :] * shrink + jnp.sum(prob, axis=1, keepdims=True)
        weights[part, :] = (prob / total[:, :span]).astype(jnp.bfloat16)
        base[part, :] = acc_old[part, :] * shrink / total


def land_values_kernel(masks, part_out, weights, base, land_mask, mine_mask, *refs):
    pieces = refs[: len(masks)]
    out_hbm, landed_hbm, out, landed, o_new, sems = refs[len(masks) :]
    steps = out.shape[0]
    rows = steps * SHARE
    place_pages(land_mask, [(piece, line) for piece in pieces for line in range(2)], landed)
    copies = [pltpu.make_async_copy(landed, landed_hbm, sems.at[steps])]
    copies[0].start()
    for g in range(0, KVH, 2):
        acc = jnp.dot(
            weights[pl.ds(g * rows, 2 * rows), :], landed[:, pl.ds(g * HD, 2 * HD)],
            preferred_element_type=jnp.float32,
        )
        first, second = pl.ds(g * rows, rows), pl.ds((g + 1) * rows, rows)
        o_new[first, :] = base[first, :] + acc[:rows, :HD]
        o_new[second, :] = base[second, :] + acc[rows:, HD:]
    mine = mine_mask[...] > 0
    for s in range(steps):
        for g in range(KVH):
            for e in range(SHARE):
                lanes = pl.ds((g * SHARE + e) * HD, HD)
                fresh = o_new[pl.ds(g * rows + s * SHARE + e, 1), :]
                tile = part_out[s, :, lanes].astype(jnp.float32)
                out[s, :, lanes] = jnp.where(mine, fresh, tile).astype(jnp.bfloat16)
        copies.append(pltpu.make_async_copy(out.at[s], out_hbm.at[s], sems.at[s]))
        copies[-1].start()
    for copy in copies:
        copy.wait()


def per_device(
    queries, new_keys, new_values, pool_keys, pool_values, page_table, cached_len,
    turn_keys, turn_values, turn_lengths, turn_slot,
):
    chain = lax.axis_size("seq")
    steps, slots, _ = queries.shape
    page_rows, width = pool_keys.shape[1:]
    pages = page_table.shape[1]
    laps = turn_keys.shape[0]
    most_pages = -(-MOSTT // page_rows)
    half = chain // 2
    assert chain & (chain - 1) == 0 and most_pages <= half
    masks = tuple(range(0, half, 2))
    rows = steps * SHARE

    def swap(x, mask):
        return lax.ppermute(x, "seq", [(i, i ^ mask) for i in range(chain)])

    def kernel(body, **settings):
        def call(*args):
            return pl.pallas_call(body, **settings)(*args)

        return call

    place = lax.axis_index("seq").reshape(1).astype(jnp.int32)

    f32, bf16 = jnp.float32, jnp.bfloat16
    block = KVH * rows
    stats = jax.ShapeDtypeStruct((block, HD), f32)
    all_rows = pltpu.VMEM((slots * block, HD), f32)
    fresh = (steps * KVH * slots, HD)
    own_k = turn_keys.reshape(laps, page_rows, width)
    own_v = turn_values.reshape(laps, page_rows, width)

    def in_hbm(*arrays):
        return tuple(pltpu.with_memory_space_constraint(x, pltpu.HBM) for x in arrays)

    got_k = swap(own_k, half)
    twin_v = swap(own_v, 1)
    large = in_hbm(queries, new_keys, new_values, pool_keys, pool_values)
    ints = in_hbm(turn_lengths, turn_slot)
    more_ints = in_hbm(page_table, cached_len)
    q_all, new_all, s_new, k_buf, v_buf, *tables = kernel(
        functools.partial(prepare_kernel, chain, masks, laps, len(ints)),
        out_shape=(
            jax.ShapeDtypeStruct((slots * block, HD), f32),
            jax.ShapeDtypeStruct((2, *fresh), f32),
            jax.ShapeDtypeStruct((slots * block, fresh[0]), f32),
            jax.ShapeDtypeStruct(pool_keys.shape, bf16),
            jax.ShapeDtypeStruct(pool_values.shape, bf16),
            jax.ShapeDtypeStruct((len(masks) * 4 * laps, page_rows, HD), bf16),
            jax.ShapeDtypeStruct((len(masks) * 4 * laps, page_rows, HD), bf16),
            jax.ShapeDtypeStruct((most_pages, 2 * len(masks), page_rows, HD), bf16),
            jax.ShapeDtypeStruct((2 * rows, HD), f32),
            jax.ShapeDtypeStruct((slots, HD), f32),
        ),
        in_specs=[SMEM] + [HBM] * 7,
        out_specs=(VMEM,) * 10,
        scratch_shapes=[
            *(pltpu.VMEM(x.shape, bf16) for x in large[:3]),
            *(pltpu.SMEM(x.shape, jnp.int32) for x in ints),
            *(pltpu.SMEM((chain,), jnp.int32) for _ in range(4)),
            pltpu.SemaphoreType.DMA((7,)),
        ],
        compiler_params=pltpu.CompilerParams(vmem_limit_bytes=16 * 2**20),
    )(place, *ints, *large)
    mask_k, mask_v, land_mask, bias, mine_mask = tables
    own_v, q_all = lax.optimization_barrier((own_v, q_all))
    got_v = swap(own_v, half)
    part_out, q_mine, acc, top, total = kernel(
        resident_kernel,
        out_shape=(
            jax.ShapeDtypeStruct(queries.shape, bf16),
            jax.ShapeDtypeStruct((block, 2 * HD), bf16),
            stats, stats, stats,
        ),
        in_specs=[SMEM] + [HBM] * 4 + [VMEM] * 5,
        out_specs=(VMEM,) * 5,
        scratch_shapes=[
            *(pltpu.SMEM(x.shape, jnp.int32) for x in ints + more_ints),
            pltpu.VMEM((slots * block, HD), bf16),
            all_rows, all_rows, all_rows,
            pltpu.SemaphoreType.DMA((4,)),
        ],
        compiler_params=pltpu.CompilerParams(vmem_limit_bytes=16 * 2**20),
        cost_estimate=pl.CostEstimate(
            flops=4 * slots * block * pages * page_rows * HD,
            bytes_accessed=2 * pool_keys.size * 2, transcendentals=0,
        ),
    )(place, *ints, *more_ints, q_all, new_all, s_new, k_buf, v_buf)

    piece = jax.ShapeDtypeStruct((2, page_rows, width), bf16)
    small = pltpu.CompilerParams(vmem_limit_bytes=8 * 2**20)

    def pick(places, *operands):
        return kernel(
            functools.partial(pick_kernel, laps, places),
            out_shape=(piece,) * len(places),
            in_specs=[VMEM] * len(operands),
            out_specs=(VMEM,) * len(places),
            compiler_params=small,
        )(*operands)

    def spread(picked):
        return [picked[0]] + [swap(x, mask) for x, mask in zip(picked[1:], masks[1:])]

    got_k, part_out = lax.optimization_barrier((got_k, part_out))
    every = tuple(range(len(masks)))
    pieces_k = spread(pick(every, mask_k, own_k, got_k))
    sources = (mask_v, own_v, got_v, twin_v, swap(got_v, 1))
    (farthest,) = pick(every[-1:], *sources)
    pieces_v = spread([*pick(every[:-1], *sources), farthest])
    joined = kernel(
        join_kernel,
        out_shape=jax.ShapeDtypeStruct((len(masks), page_rows, width), bf16),
        in_specs=[VMEM] * len(masks),
        out_specs=VMEM,
        compiler_params=small,
    )(*pieces_k)
    other_k = swap(joined, 1)

    span = most_pages * page_rows
    landed_k, weights, base = kernel(
        functools.partial(land_keys_kernel, masks),
        out_shape=(
            jax.ShapeDtypeStruct((span, width), bf16),
            jax.ShapeDtypeStruct((block, span), bf16),
            stats,
        ),
        in_specs=[VMEM] * (7 + len(masks)),
        out_specs=(VMEM,) * 3,
        compiler_params=small,
    )(q_mine, acc, top, total, land_mask, bias, *pieces_k, other_k)
    attended, landed_v = kernel(
        functools.partial(land_values_kernel, masks),
        out_shape=(
            jax.ShapeDtypeStruct(queries.shape, bf16), jax.ShapeDtypeStruct((span, width), bf16)
        ),
        in_specs=[VMEM] * (5 + len(masks)),
        out_specs=(HBM, HBM),
        scratch_shapes=[
            pltpu.VMEM(queries.shape, bf16),
            pltpu.VMEM((span, width), bf16),
            pltpu.VMEM((block, HD), f32),
            pltpu.SemaphoreType.DMA((steps + 1,)),
        ],
        compiler_params=small,
    )(part_out, weights, base, land_mask, mine_mask, *pieces_v)
    return attended, landed_k[None], landed_v[None]


def solution(mesh):
    both = ("groups", "seq")
    in_specs = (
        P(None, both, None),
        P(None, both, None),
        P(None, both, None),
        P(both, None, None),
        P(both, None, None),
        P(both, None),
        P(both),
        P(None, both, None, None),
        P(None, both, None, None),
        P("groups"),
        P("groups"),
    )
    out_specs = (P(None, both, None), P(both, None, None), P(both, None, None))
    return jax.shard_map(
        per_device, mesh=mesh, in_specs=in_specs, out_specs=out_specs, check_vma=False
    )
```
